128 devices in a mesh: dp: 16 (over y, z), tensor: 8 (over x, core).
Axes of the slice: x: 4, y: 4, z: 4, core: 2. Of those that a mesh axis runs over, the one named last changes fastest.
Arguments:
- hidden: bfloat16 [3072, 4096], P('dp'), may hold values from -64 to 64
- output_weight: bfloat16 [4096, 128256], P(None, ('dp', 'tensor')), may hold values from -0.109375 to 0.109375
- targets: int32 [3072], P('dp'), may hold values from 0 to 128255
- labels: int32 [3072, 1], P('dp'), may hold values from 0 to 63; in each aligned block of 192 rows (0 to 191, 192 to 383, ...) at most 12 rows name the same one
- prev_scores: float32 [64], P('dp'), may hold values from -12 to 320
- prev_probs: float32 [64], P('dp')
- next_domains: int32 [256], P('dp'), may hold values from 0 to 63
Outputs:
- token_loss: float32 [3072], P(('dp', 'tensor'))
- new_scores: float32 [64], P('dp')
- log_probs: float32 [64], replicated
- sample_weights: float32 [256], P('dp')
The draws below stay inside these ranges and needn't reach their ends.
Inputs may be any that keep to these rules, and one draw needn't show every extreme that they name: `labels`: within the 192 tokens of one index of dp no domain appears more than 12 times; every domain appears somewhere in the batch.
All inputs are finite; a program needn't handle non-finite values.
Results may differ from the reference program's by a relative error of at most 0.0003.
Values may be sent and summed in bfloat16 or wider, within the bound.
A program may use at most 128 MiB of HBM per device.

```python
import math
import jax
import jax.numpy as jnp
import numpy as np
from jax import lax

D = 4096
V = 128256
K = 64
STEP = 2000
TOK_DEV = 192
CAP = 12
TOKENS = 3072
NEXT = 256


def weight_columns(key, columns):
    bound = 7.0 * D ** (-0.5)
    drawn = jax.vmap(lambda column: jax.random.normal(jax.random.fold_in(key, column), (D,), jnp.float32))(columns)
    return jnp.clip(drawn * D ** (-0.5), -bound, bound)


def draw_output_weight(key, part):
    columns = jnp.arange(V, dtype=jnp.int32)
    return weight_columns(jax.random.fold_in(key, 11), columns).T.astype(jnp.bfloat16)


def draw_hidden(key, part):
    index_rows = jnp.arange(TOKENS, dtype=jnp.int32)
    rising = 3.0 ** (index_rows.astype(jnp.float32) / TOKENS)
    base = jax.random.normal(jax.random.fold_in(key, 23), (TOKENS, D), jnp.float32)
    scales = 0.6 * rising * jnp.exp(jax.random.uniform(jax.random.fold_in(key, 29), (TOKENS,), jnp.float32, -0.35, 0.35))
    result = base * scales[:, None]
    return jnp.clip(result, -64.0, 64.0).astype(jnp.bfloat16)


def draw_prev_scores(key, part):
    noise = jax.random.normal(jax.random.fold_in(key, 41), (K,), jnp.float32)
    values = 2.0 * noise
    return jnp.clip(values, -12.0, 320.0)


def draw_prev_probs(key, part):
    earlier = min(1.0 / K, math.sqrt(math.log(K) / (K * (STEP - 1))))
    logits = 1.5 * jax.random.normal(jax.random.fold_in(key, 43), (K,), jnp.float32)
    return earlier + (1.0 - K * earlier) * jax.nn.softmax(logits)


def plant(values, stream_key, least, high):
    index_at = [jax.random.randint(jax.random.fold_in(stream_key, axis), (), 0, length) for axis, length in enumerate(values.shape)]
    widest = values.shape.index(max(values.shape))
    beside = index_at[:widest] + [(index_at[widest] + 1) % values.shape[widest]] + index_at[widest + 1:]
    return values.at[tuple(index_at)].set(least).at[tuple(beside)].set(high)


def shared_out(rng, own, number, rows, number_of, top, limit, skew):
    sequence = jax.random.permutation(rng, number_of)
    crowded, common = shares(number_of, rows * top, limit, skew, True), shares(number_of, rows * top, limit, skew, False)
    places = jnp.arange(number_of)

    def named(sizes, offset_by):
        used = int((sizes > 0).sum())
        fixed = max(1, used // 4)
        passed = fixed + (places - fixed + offset_by * (used - fixed)) % max(1, number_of - fixed)
        return jnp.zeros((number_of,), jnp.int32).at[sequence[jnp.where(places < fixed, places, passed)]].set(jnp.asarray(sizes, jnp.int32))

    sizes = jnp.where(number % 4 == 0, named(crowded, number // 4), named(common, number - number // 4 - 1))
    mixed = jax.random.permutation(jax.random.fold_in(own, 3), number_of)
    source_of, taker = mixed[0:number_of // 2 * 2:2], mixed[1:number_of // 2 * 2:2]
    margin = jnp.minimum(sizes[source_of] - 1, limit - sizes[taker]) // 2
    margin = jnp.where((source_of == sequence[0]) | (taker == sequence[0]) | (sizes[taker] == 0), 0, jnp.maximum(margin, 0))
    passed = jax.random.randint(jax.random.fold_in(own, 4), (number_of // 2,), 0, 1 << 20) % (margin + 1)
    sizes = sizes.at[source_of].add(-passed).at[taker].add(passed)
    items = jnp.searchsorted(jnp.cumsum(sizes), jnp.arange(rows * top), side="right").astype(jnp.int32)
    grid = items.reshape(top, rows).T
    grid = grid[jax.random.permutation(jax.random.fold_in(own, 1), rows)]
    offset_by = jax.random.randint(jax.random.fold_in(own, 2), (rows, 1), 0, top)
    return jnp.take_along_axis(grid, (jnp.arange(top)[None, :] + offset_by) % top, axis=1)


def shares(number_of, total, limit, skew, full):
    loads = [(1 << 20) // math.isqrt(standing ** skew) + 1 for standing in range(1, number_of + 1)]
    largest = limit if full else min(limit, max(-(-total // number_of), total * loads[0] // sum(loads)))
    least = 1 if total - largest >= number_of - 1 else 0
    given, rest = [largest] + [least] * (number_of - 1), total - largest - least * (number_of - 1)
    while rest > 0:
        candidates = [i for i in range(1, number_of) if given[i] < largest] or [i for i in range(1, number_of) if given[i] < limit]
        pool, budget = sum([loads[i] for i in candidates]), rest
        for i in candidates:
            extra = min(limit - given[i], max(1, budget * loads[i] // pool), rest)
            given[i] = given[i] + extra
            rest = rest - extra
    return np.array(given)


def setup_inputs(seed: int = 0) -> dict:
    key_of = jax.random.split(jax.random.key(seed), 8)
    hidden = draw_hidden(jax.random.fold_in(key_of[7], 71), 0)
    output_weight = draw_output_weight(jax.random.fold_in(key_of[7], 71), 0)
    targets = plant(jax.random.randint(key_of[2], (TOKENS,), 0, V), jax.random.fold_in(key_of[2], 1), 0, V - 1).astype(jnp.int32)
    labels_keys = jax.random.split(jax.random.fold_in(key_of[3], 1), TOKENS // TOK_DEV)
    labels_turns = jax.random.permutation(jax.random.fold_in(key_of[3], 3), TOKENS // TOK_DEV)
    labels = jax.vmap(lambda own, number: shared_out(jax.random.fold_in(key_of[3], 2), own, number, TOK_DEV, K, 1, CAP, 2))(labels_keys, labels_turns).reshape((TOKENS, 1))
    prev_scores = draw_prev_scores(jax.random.fold_in(key_of[7], 71), 0)
    prev_probs = draw_prev_probs(jax.random.fold_in(key_of[7], 71), 0)
    next_domains = plant(jax.random.randint(key_of[6], (NEXT,), 0, K), jax.random.fold_in(key_of[6], 1), 0, K - 1).astype(jnp.int32)
    return dict(hidden=hidden, output_weight=output_weight, targets=targets, labels=labels, prev_scores=prev_scores, prev_probs=prev_probs, next_domains=next_domains)


def exploration_rates():
    earlier = min(1.0 / K, math.sqrt(math.log(K) / (K * (STEP - 1))))
    current = min(1.0 / K, math.sqrt(math.log(K) / (K * STEP)))
    return (earlier, current)

def reference(hidden, output_weight, targets, labels, prev_scores, prev_probs, next_domains):
    block_size = math.gcd(TOKENS, 256)

    def block_loss(pair):
        row_block, wanted = pair
        logits = jnp.dot(row_block, output_weight, preferred_element_type=jnp.float32)
        largest = lax.optimization_barrier(jnp.max(logits, axis=1))
        expsum = lax.optimization_barrier(jnp.sum(jnp.exp(logits - largest[:, None]), axis=1))
        picked = jnp.take_along_axis(logits, wanted[:, None], axis=1)[:, 0]
        return largest + jnp.log(expsum) - picked
    token_loss = lax.map(block_loss, (hidden.reshape(TOKENS // block_size, block_size, D), targets.reshape(TOKENS // block_size, block_size))).reshape(TOKENS)
    onehot = (labels[:, 0:1] == jnp.arange(K, dtype=jnp.int32)[None, :]).astype(jnp.float32)
    totals = jnp.dot(token_loss, onehot, precision=lax.Precision.HIGHEST)
    counts = lax.optimization_barrier(jnp.sum(onehot, axis=0))
    earlier, current = exploration_rates()
    new_scores = current / earlier * prev_scores + current * (totals / counts) / prev_probs
    largest_score = jnp.max(new_scores)
    weights = jnp.exp(new_scores - largest_score)
    probs = (1.0 - K * current) * (weights / jnp.sum(weights)) + current
    log_probs = jnp.log(probs)
    chosen = lax.optimization_barrier(jnp.sum(jnp.where(next_domains[:, None] == jnp.arange(K, dtype=jnp.int32)[None, :], probs[None, :], 0.0), axis=1))
    sample_weights = 1.0 / (K * chosen)
    return (token_loss, new_scores, log_probs, sample_weights)
```

```python
import functools
import math

import jax
import jax.numpy as jnp
from jax import lax
from jax.experimental import pallas as pl
from jax.experimental.pallas import tpu as pltpu
from jax.sharding import Mesh
from jax.sharding import PartitionSpec as P

K = 64
STEP = 2000
N = 4
HALF = 96
COLS = 1002
WIDE = 4096
DP = ("y", "z")
TENSOR = ("x", "c")
ALL = ("y", "z", "x", "c")
DIRS = ("+y", "-y", "+z", "-z")
F32 = jnp.float32
NT = (((1,), (1,)), ((), ()))
CUT = 512


ORDER = [
    (0, 0), (0, 1), (0, 3), (1, 0), (3, 0), (1, 3), (3, 1), (1, 1),
    (3, 3), (0, 2), (2, 0), (1, 2), (2, 1), (2, 3), (3, 2), (2, 2),
]
POS = {s: k for k, s in enumerate(ORDER)}
LAST_SLOT = [2, 5, 7, 10, 13, 15]
GROUPS = len(LAST_SLOT)
ROWS_G = 256
N_W = 8


def group_of(slot):
    return next(g for g, k in enumerate(LAST_SLOT) if slot <= k)


def moved(n, d):
    k = 1 if d[0] == "+" else -1
    return ((n[0] + (k if d[1] == "y" else 0)) % N, (n[1] + (k if d[1] == "z" else 0)) % N)


def neg(n):
    return ((-n[0]) % N, (-n[1]) % N)


def children(rot, n):
    axis, sign = rot // 2, 1 - 2 * (rot % 2)
    a, b = n if axis == 0 else n[::-1]
    a, b = (a * sign) % N, (b * sign) % N
    first, second = ("y", "z") if axis == 0 else ("z", "y")
    fwd, back = ("+", "-") if sign == 1 else ("-", "+")
    out = []
    if b == 0:
        if a in (0, 1):
            out.append(fwd + first)
        if a == 0:
            out.append(back + first)
    if b in (0, 1):
        out.append(fwd + second)
    if b == 0:
        out.append(back + second)
    return out


def x_dir(rot):
    return "+x" if rot < 2 else "-x"


def due(role, rot, n, hop, step):
    own = step * (group_of(POS[neg(n)]) + 1)
    out = own
    for d in children(rot, n):
        out = min(out, due(role, rot, moved(n, d), hop, step) - hop)
    if role == "M" and n != (0, 0):
        out = min(out, own - hop)
    return out


def plan(T=1.45, L=2.1, hop=4.5, step=4.0, half=1.32, horizon=1.6, w_ready=15.0, t0=1.2):
    here = {((0, 0), role, rot): 0.0 for role in "CMO" for rot in range(4)}
    todo = {d: [] for d in DIRS + ("+x", "-x")}
    for role in "CM":
        for rot in range(4):
            for n in ORDER:
                for d in children(rot, n):
                    todo[d].append((due(role, rot, moved(n, d), hop, step), neg(n), role, rot))
                if role == "M" and n != (0, 0):
                    late = step * (group_of(POS[neg(n)]) + 1)
                    todo[x_dir(rot)].append((late, neg(n), role, rot))
    end = {d: 0.0 for d in todo}
    chunks = [(g, w) for g in range(GROUPS) for w in range(2)]
    program, t, w_sent = [], t0, 0

    def service(t):
        nonlocal w_sent
        if w_sent < N_W:
            program.append(("w", w_sent))
            w_sent += 1
        for d in todo:
            while end[d] < t + horizon:
                ready = [
                    (late, here[s, role, rot], s, role, rot)
                    for late, s, role, rot in todo[d]
                    if here.get((s, role, rot), 1e9) <= t
                ]
                if not ready:
                    break
                late, _, s, role, rot = min(ready)
                todo[d].remove((late, s, role, rot))
                end[d] = max(t + 0.05, end[d]) + T
                if d[1] == "x":
                    here[s, "O", rot] = end[d] + L
                else:
                    here[neg(moved(neg(s), d)), role, rot] = end[d] + L
                program.append(("send", d, role, rot, s))

    def ready_at(g, w):
        last = max(
            here.get((s, role, rot), 1e9)
            for s in ORDER[: LAST_SLOT[g] + 1]
            for role in "CMO"
            for rot in range(4)
        )
        return max(last, w_ready if w else 3.5)

    while any(todo.values()) or chunks:
        service(t)
        now = [c for c in chunks if ready_at(*c) <= t]
        if now:
            chunks.remove(now[0])
            program.append(("half", *now[0], 0))
            t += half
            service(t)
            program.append(("half", *now[0], 1))
            t += half
        else:
            later = [v for v in here.values() if t < v < 1e8]
            later += [e - horizon for e in end.values() if e - horizon > t]
            later += [v for v in (ready_at(*c) for c in chunks) if t < v < 1e8]
            t = min(later) + 0.01
    return program


def segments():
    have = {((0, 0), role, rot) for role in "CMO" for rot in range(4)}
    done, flags, told = [], set(), 0
    parts, ops = [], []
    ready_stats = []

    def need(s, role, rot):
        if (s, role, rot) not in have:
            have.add((s, role, rot))
            ops.append(("wait", s, role, rot))

    for op in plan():
        if op[0] == "send":
            need(op[4], op[2], op[3])
            ops.append(op)
        elif op[0] == "w":
            ops.append(op)
        else:
            _, g, w, h = op
            if h == 0:
                if "meta" not in flags:
                    flags.add("meta")
                    ops.append(("meta",))
                if w not in flags:
                    flags.add(w)
                    ops.append(("w_wait", w))
                for s in ORDER[: LAST_SLOT[g] + 1]:
                    for role in "CMO":
                        for rot in range(4):
                            need(s, role, rot)
                done.append((g, w))
            parts.append(ops)
            ops = ready_stats
            ready_stats = []
            if h == 1:
                both = [k for k in range(GROUPS) if (k, 0) in done and (k, 1) in done]
                while told < len(both) and both[told] == told:
                    ops.append(("merge", told))
                    lo = 8 * told
                    for k in range(16):
                        if 3 * k + 2 < lo + 8 and 3 * k + 2 >= lo:
                            ops.append(("stat", k))
                            ready_stats.append(("stat_send", k))
                    told += 1
    parts.append(ops)
    parts[-1] += ready_stats
    return done, parts


def rates():
    earlier = min(1.0 / K, math.sqrt(math.log(K) / (K * (STEP - 1))))
    current = min(1.0 / K, math.sqrt(math.log(K) / (K * STEP)))
    return earlier, current


def sum_lanes(v):
    return jnp.sum(v, axis=1, keepdims=True)


def kernel(
    hid, wt, tgt, lab, psc, ppr, nxt,
    o_loss, o_score, o_log, o_weight,
    hbuf, wbuf, meta_out, meta_in, two, trow, cols, sbuf, merged, st_out, st_in, xs_out, xs_in, lo_out, lo_in,
    h_load, w_load, h_send, h_recv, w_send, w_recv, meta_send, meta_recv, st_send, st_recv, xs_send, xs_recv,
    lo_send, lo_recv,
):
    my, mz, mx, mc = (lax.axis_index(a) for a in ALL)
    par = lax.rem(mx, 2)

    def device(dy=0, dz=0, dx=0, dc=0):
        return {
            "y": lax.rem(my + dy, N),
            "z": lax.rem(mz + dz, N),
            "x": lax.rem(mx + dx, N),
            "c": lax.rem(mc + dc, 2),
        }

    def remote(src, dst, send, recv, to):
        return pltpu.make_async_remote_copy(
            src_ref=src, dst_ref=dst, send_sem=send, recv_sem=recv, device_id=to,
            device_id_type=pl.DeviceIdType.MESH,
        )

    def wait_for(ref, sem):
        pltpu.make_async_copy(ref, ref, sem).wait()

    loads = []
    for rg in range(3):
        for kq in range(4):
            rows = pl.ds(pl.multiple_of(mc * HALF + rg * 32, 32), 32)
            loads.append(
                pltpu.make_async_copy(
                    hid.at[rows, pl.ds(kq * 1024, 1024)], hbuf.at[POS[0, 0] * 3 + rg, kq], h_load.at[rg * 4 + kq]
                )
            )
    for load in loads:
        load.start()
    own_w = pltpu.make_async_copy(wt, wbuf.at[0], w_load)
    own_w.start()

    barrier = pltpu.get_barrier_semaphore()
    plane = [(dy, dz, dc) for dy in range(N) for dz in range(N) for dc in range(2) if (dy, dz, dc) != (0, 0, 0)]
    for dy, dz, dc in plane:
        pl.semaphore_signal(barrier, inc=1, device_id=device(dy, dz, 0, dc), device_id_type=pl.DeviceIdType.MESH)
    for dx in range(1, N):
        pl.semaphore_signal(barrier, inc=1, device_id=device(0, 0, dx), device_id_type=pl.DeviceIdType.MESH)

    lane = lax.broadcasted_iota(jnp.int32, (8, 128), 1)
    two[...] = jnp.zeros_like(two)
    two[0:1, 0:192] = tgt[...]
    two[1:2, 0:192] = lab[...]
    both = two[...]
    first = jnp.where(lane < HALF, both[:, :128], -1).astype(F32)
    second = jnp.where(lane < HALF, pltpu.roll(both, 256 - HALF, 1)[:, :128], -1).astype(F32)
    meta_out[...] = jnp.zeros_like(meta_out)
    meta_out[0:1] = jnp.where(mc == 0, first[0:1], second[0:1])
    meta_out[1:2] = first[1:2]
    meta_out[2:3] = second[1:2]
    meta_out[3:4, 0:4] = psc[...]
    meta_out[4:5, 0:4] = ppr[...]
    meta_in[POS[0, 0]] = meta_out[...]
    for load in loads:
        load.wait()
    pl.semaphore_wait(barrier, len(plane) + N - 1)

    for s in ORDER[1:]:
        k = POS[neg(s)]
        remote(meta_out, meta_in.at[k], meta_send, meta_recv.at[k], device(s[0], s[1])).start()

    def piece(slot, role, rot):
        rg = {"C": 0, "M": 1 + par, "O": 2 - par}[role]
        return hbuf.at[slot * 3 + rg, rot], (slot * 3 + rg, rot)

    half_sub = lax.broadcasted_iota(jnp.int32, (K, 128), 0)
    half_lane = lax.broadcasted_iota(jnp.int32, (K, 128), 1)

    def do_meta():
        for k in range(1, 16):
            wait_for(meta_in.at[k], meta_recv.at[k])
        wide_lane = lax.broadcasted_iota(jnp.int32, (8, 256), 1)
        rows = [jnp.zeros((8, 256), F32) for _ in range(GROUPS)]
        counts = jnp.zeros((K, 128), F32)
        score = jnp.zeros((K, 128), F32)
        prob = jnp.zeros((K, 128), F32)
        for k, s in enumerate(ORDER):
            tile = meta_in[k]
            wide = jnp.concatenate([tile, tile], axis=1)
            at = 3 * k
            g, off = at // 8, 32 * (at % 8)
            n = min(3, 8 - at % 8)
            turned = pltpu.roll(wide, off, 1) if off else wide
            rows[g] = jnp.where((wide_lane >= off) & (wide_lane < off + 32 * n), turned, rows[g])
            if n < 3:
                turned = pltpu.roll(wide, 256 - 32 * n, 1)
                rows[g + 1] = jnp.where(wide_lane < 32 * (3 - n), turned, rows[g + 1])
            sub = half_sub.astype(F32)
            for r in (1, 2):
                counts += jnp.where(tile[r : r + 1] == sub, 1.0, 0.0)
            dp = lax.rem(my + s[0], N) * N + lax.rem(mz + s[1], N)
            mine = (half_lane == half_sub - 4 * dp) & (half_lane < 4)
            score += jnp.where(mine, tile[3:4], 0.0)
            prob += jnp.where(mine, tile[4:5], 0.0)
        for g in range(GROUPS):
            trow[g] = rows[g].astype(jnp.int32)
        for i, v in enumerate((counts, score, prob)):
            cols[i] = jnp.broadcast_to(sum_lanes(v), (K, 128))

    def run(ops):
        for op in ops:
            if op[0] == "wait":
                _, s, role, rot = op
                ref, (i, r) = piece(POS[s], role, rot)
                wait_for(ref, h_recv.at[i, r])
            elif op[0] == "send":
                _, d, role, rot, s = op
                src, _ = piece(POS[s], role, rot)
                step = 1 if d[0] == "+" else N - 1
                if d[1] == "x":
                    dst, (i, r) = piece(POS[s], role, rot)
                    to = device(dx=step)
                else:
                    dst, (i, r) = piece(POS[neg(moved(neg(s), d))], role, rot)
                    to = device(dy=step) if d[1] == "y" else device(dz=step)
                remote(src, dst, h_send, h_recv.at[i, r], to).start()
            elif op[0] == "w":
                rows = pl.ds(op[1] * 128, min(128, COLS - op[1] * 128))
                remote(
                    wt.at[rows], wbuf.at[1, rows], w_send.at[op[1]], w_recv.at[op[1]], device(dc=1)
                ).start()
            elif op[0] == "w_wait":
                if op[1] == 0:
                    own_w.wait()
                else:
                    for i in range(N_W):
                        rows = pl.ds(i * 128, min(128, COLS - i * 128))
                        wait_for(wbuf.at[1, rows], w_recv.at[i])
            elif op[0] == "meta":
                do_meta()
            elif op[0] == "merge":
                a, b = sbuf[op[1], 0], sbuf[op[1], 1]
                top = jnp.maximum(a[0:1], b[0:1])
                merged[op[1], 0:1] = top
                merged[op[1], 1:2] = a[1:2] * jnp.exp(a[0:1] - top) + b[1:2] * jnp.exp(b[0:1] - top)
                merged[op[1], 2:3] = a[2:3] + b[2:3]
            elif op[0] == "stat":
                k = op[1]
                at = 3 * k
                g, off = at // 8, 32 * (at % 8)
                n = min(3, 8 - at % 8)
                tile = merged[g]
                msg = (pltpu.roll(tile, 256 - off, 1) if off else tile)[:, :128]
                if n < 3:
                    msg = jnp.where(lane < 32 * n, msg, pltpu.roll(merged[g + 1], 32 * n, 1)[:, :128])
                if ORDER[k] == (0, 0):
                    st_in[k] = msg
                else:
                    st_out[k] = msg
            elif op[0] == "stat_send":
                k = op[1]
                s = ORDER[k]
                if s != (0, 0):
                    i = POS[neg(s)]
                    remote(st_out.at[k], st_in.at[i], st_send, st_recv.at[i], device(s[0], s[1])).start()

    base = ((my * N + mz) * 8 + mx * 2) * COLS
    chunks, parts = segments()
    run(parts[0])

    def stats(g, w, lo, hi, target):
        rhs = jnp.concatenate([hbuf[pl.ds(8 * g, 8), kq].reshape(ROWS_G, 1024) for kq in range(4)], axis=1)
        logits = lax.dot_general(wbuf[w, lo:hi], rhs, NT, preferred_element_type=F32)
        top = jnp.max(logits, axis=0, keepdims=True)
        total = jnp.sum(jnp.exp(logits - top), axis=0, keepdims=True)
        row = lax.broadcasted_iota(jnp.int32, logits.shape, 0) + lo
        picked = jnp.sum(jnp.where(row == target, logits, 0.0), axis=0, keepdims=True)
        return top, total, picked

    def of(j, values):
        if all(v == k // 2 for k, v in enumerate(values)):
            return j // 2
        if all(v == k % 2 for k, v in enumerate(values)):
            return j % 2
        out = 0
        for k, v in enumerate(values):
            if v:
                out += jnp.where(j == k, v, 0)
        return out

    def chunk(j, _):
        for k in range(1, len(chunks)):
            if parts[2 * k]:
                pl.when(j == k)(functools.partial(run, parts[2 * k]))
        g, w = of(j, [c[0] for c in chunks]), of(j, [c[1] for c in chunks])
        core = jnp.where(w == 0, mc, 1 - mc)
        target = trow[g][0:1] - (base + core * COLS)
        a = stats(g, w, 0, CUT, target)
        for k in range(len(chunks)):
            if parts[2 * k + 1]:
                pl.when(j == k)(functools.partial(run, parts[2 * k + 1]))
        b = stats(g, w, CUT, COLS, target)
        top = jnp.maximum(a[0], b[0])
        sbuf[g, w, 0:1] = top
        sbuf[g, w, 1:2] = a[1] * jnp.exp(a[0] - top) + b[1] * jnp.exp(b[0] - top)
        sbuf[g, w, 2:3] = a[2] + b[2]
        return 0

    lax.fori_loop(0, len(chunks), chunk, 0)
    run(parts[-1])

    for k in range(1, 16):
        wait_for(st_in.at[k], st_recv.at[k])

    def joined(tiles):
        top = functools.reduce(jnp.maximum, [t[0:1] for t in tiles])
        total = functools.reduce(jnp.add, [t[1:2] * jnp.exp(t[0:1] - top) for t in tiles])
        return top, total, functools.reduce(jnp.add, [t[2:3] for t in tiles])

    for i, v in enumerate(joined([st_in[k] for k in range(16)])):
        xs_out[i : i + 1] = v
    for dx in range(1, N):
        remote(xs_out, xs_in.at[N - dx], xs_send, xs_recv.at[N - dx], device(dx=dx)).start()
    xs_in[0] = xs_out[...]
    for dx in range(1, N):
        wait_for(xs_in.at[dx], xs_recv.at[dx])
    top, total, picked = joined([xs_in[dx] for dx in range(N)])
    loss = top + jnp.log(total) - picked
    lo_out[...] = loss
    for dy, dz, dc in plane:
        i = POS[neg((dy, dz))] * 2 + dc
        remote(lo_out, lo_in.at[i], lo_send, lo_recv.at[i], device(dy, dz, 0, dc)).start()
    lo_in[0] = lo_out[...]
    for i in range(1, 32):
        wait_for(lo_in.at[i], lo_recv.at[i])

    sums = jnp.zeros((K, 128), F32)
    sub = half_sub.astype(F32)
    for k in range(16):
        tile = meta_in[k]
        for dc in range(2):
            labels = jnp.where(lax.rem(mc + dc, 2) == 0, tile[1:2], tile[2:3])
            sums += jnp.where(labels == sub, lo_in[2 * k + dc], 0.0)
    sums = jnp.broadcast_to(sum_lanes(sums), (K, 128))
    earlier, current = rates()
    score = current / earlier * cols[1] + current * (sums / cols[0]) / cols[2]
    weight = jnp.exp(score - jnp.max(score, axis=0, keepdims=True))
    probs = (1.0 - K * current) * (weight / jnp.sum(weight, axis=0, keepdims=True)) + current
    log_probs = jnp.log(probs)
    dp = my * N + mz

    def across(mask, v):
        return jnp.sum(jnp.where(mask, v, 0.0), axis=0, keepdims=True)

    o_score[...] = across(half_lane == half_sub - 4 * dp, score)[:, :4]
    o_log[...] = across(half_lane == half_sub, log_probs)[:, :K]
    two[2:3, 0:16] = nxt[...]
    chosen = across(two[2:3, :128] == half_sub, probs)
    o_weight[...] = (1.0 / (K * chosen))[:, :16]
    loss = jnp.where(mx // 2 == mc, lo_in[0], lo_in[1])
    loss = jnp.broadcast_to(loss, (8, 128))
    out = loss
    for q in range(1, 4):
        out = jnp.where(2 * lax.rem(mx, 2) + mc == q, pltpu.roll(loss, 128 - 24 * q, 1), out)
    o_loss[...] = out[0:1, :24]

    wait_for(hbuf.at[pl.ds(0, 45)], h_send)
    for i in range(N_W):
        rows = pl.ds(i * 128, min(128, COLS - i * 128))
        wait_for(wbuf.at[1, rows], w_send.at[i])
    wait_for(meta_in.at[pl.ds(0, 15)], meta_send)
    wait_for(st_in.at[pl.ds(0, 15)], st_send)
    wait_for(xs_in.at[pl.ds(0, 3)], xs_send)
    wait_for(lo_in.at[pl.ds(0, 31)], lo_send)


def body(hidden, output_weight, targets, labels, prev_scores, prev_probs, next_domains):
    dma = pltpu.SemaphoreType.DMA
    vmem = pl.BlockSpec(memory_space=pltpu.VMEM)
    outs = pl.pallas_call(
        kernel,
        out_shape=[jax.ShapeDtypeStruct((1, n), F32) for n in (24, 4, K, 16)],
        in_specs=[pl.BlockSpec(memory_space=pl.ANY)] * 2 + [vmem] * 5,
        out_specs=[vmem] * 4,
        scratch_shapes=[
            pltpu.VMEM((48, 4, 32, 1024), jnp.bfloat16),
            pltpu.VMEM((2, COLS, WIDE), jnp.bfloat16),
            pltpu.VMEM((8, 128), F32),
            pltpu.VMEM((16, 8, 128), F32),
            pltpu.VMEM((8, 256), jnp.int32),
            pltpu.VMEM((GROUPS, 8, 256), jnp.int32),
            pltpu.VMEM((3, K, 128), F32),
            pltpu.VMEM((GROUPS, 2, 8, 256), F32),
            pltpu.VMEM((GROUPS, 8, 256), F32),
            pltpu.VMEM((16, 8, 128), F32),
            pltpu.VMEM((16, 8, 128), F32),
            pltpu.VMEM((8, 128), F32),
            pltpu.VMEM((N, 8, 128), F32),
            pltpu.VMEM((1, 128), F32),
            pltpu.VMEM((32, 1, 128), F32),
            dma((12,)),
            dma(()),
            dma(()),
            dma((48, 4)),
            dma((N_W,)),
            dma((N_W,)),
            dma(()),
            dma((16,)),
            dma(()),
            dma((16,)),
            dma(()),
            dma((N,)),
            dma(()),
            dma((32,)),
        ],
        compiler_params=pltpu.CompilerParams(
            collective_id=0, has_side_effects=True, vmem_limit_bytes=56 * 1024 * 1024
        ),
    )(
        hidden,
        output_weight.T,
        targets.reshape(1, -1),
        labels.reshape(1, -1),
        prev_scores.reshape(1, -1),
        prev_probs.reshape(1, -1),
        next_domains.reshape(1, -1),
    )
    return tuple(o.reshape(-1) for o in outs)


def solution(mesh):
    torus = Mesh(mesh.devices.reshape(N, N, N, 2), ALL)
    return jax.shard_map(
        body,
        mesh=torus,
        in_specs=(P(DP, None), P(None, ALL), P(DP), P(DP, None), P(DP), P(DP), P(DP)),
        out_specs=(P(ALL), P(DP), P(), P(DP)),
        check_vma=False,
    )
```

```python
import functools
import math

import jax
import jax.numpy as jnp
from jax import lax
from jax.experimental import pallas as pl
from jax.experimental.pallas import tpu as pltpu
from jax.sharding import Mesh
from jax.sharding import PartitionSpec as P

K = 64
STEP = 2000
N = 4
HALF = 96
COLS = 1002
WIDE = 4096
DP = ("y", "z")
TENSOR = ("x", "c")
ALL = ("y", "z", "x", "c")
DIRS = ("+y", "-y", "+z", "-z")
F32 = jnp.float32
NT = (((1,), (1,)), ((), ()))
SPLIT = 2


ORDER = [
    (0, 0), (0, 1), (0, 3), (1, 0), (3, 0), (1, 3), (3, 1), (1, 1),
    (3, 3), (0, 2), (2, 0), (1, 2), (2, 1), (2, 3), (3, 2), (2, 2),
]
POS = {s: k for k, s in enumerate(ORDER)}
LAST_SLOT = [2, 5, 7, 10, 13, 15]
GROUPS = len(LAST_SLOT)
ROWS_G = 256
N_W = 8
FAR = (2, 2)


def group_of(slot):
    return next(g for g, k in enumerate(LAST_SLOT) if slot <= k)


def moved(n, d):
    k = 1 if d[0] == "+" else -1
    return ((n[0] + (k if d[1] == "y" else 0)) % N, (n[1] + (k if d[1] == "z" else 0)) % N)


def before(n, d):
    return moved(n, ("-" if d[0] == "+" else "+") + d[1])


def opposite(s):
    return ((s[0] + 2) % N, (s[1] + 2) % N)


def neg(n):
    return ((-n[0]) % N, (-n[1]) % N)


def children(rot, n):
    axis, sign = rot // 2, 1 - 2 * (rot % 2)
    a, b = n if axis == 0 else n[::-1]
    a, b = (a * sign) % N, (b * sign) % N
    first, second = ("y", "z") if axis == 0 else ("z", "y")
    fwd, back = ("+", "-") if sign == 1 else ("-", "+")
    out = []
    if b == 0:
        if a in (0, 1):
            out.append(fwd + first)
        if a == 0:
            out.append(back + first)
    if b in (0, 1):
        out.append(fwd + second)
    if b == 0:
        out.append(back + second)
    return out


def x_dir(rot):
    return "+x" if rot < 2 else "-x"


def due(role, rot, n, hop, step):
    own = step * (group_of(POS[neg(n)]) + 1)
    out = own
    for d in children(rot, n):
        out = min(out, due(role, rot, moved(n, d), hop, step) - hop)
    if role == "M" and n not in ((0, 0), FAR):
        out = min(out, own - hop)
    return out


def plan(T=1.45, L=2.1, hop=4.5, step=4.0, chunk=2.6, horizon=1.6, w_ready=15.0, t0=1.2):
    here = {((0, 0), role, rot): 0.0 for role in "CMO" for rot in range(4)}
    todo = {d: [] for d in DIRS + ("+x", "-x")}
    for role in "CM":
        for rot in range(4):
            for n in ORDER:
                for d in children(rot, n):
                    todo[d].append((due(role, rot, moved(n, d), hop, step), neg(n), role, rot))
                if role == "M" and n not in ((0, 0), FAR):
                    late = step * (group_of(POS[neg(n)]) + 1)
                    todo[x_dir(rot)].append((late, neg(n), role, rot))
    for rot, d in enumerate(DIRS):
        todo[d].append((step * GROUPS, neg(before(FAR, d)), "O", rot))
    end = {d: 0.0 for d in todo}
    chunks = [(g, w) for g in range(GROUPS) for w in range(2)]
    program, t, w_sent = [], t0, 0

    def service(t):
        nonlocal w_sent
        if w_sent < N_W:
            program.append(("w", w_sent))
            w_sent += 1
        for d in todo:
            while end[d] < t + horizon:
                ready = [
                    (late, here[s, role, rot], s, role, rot)
                    for late, s, role, rot in todo[d]
                    if here.get((s, role, rot), 1e9) <= t
                ]
                if not ready:
                    break
                late, _, s, role, rot = min(ready)
                todo[d].remove((late, s, role, rot))
                end[d] = max(t + 0.05, end[d]) + T
                if d[1] == "x":
                    here[s, "O", rot] = end[d] + L
                else:
                    here[neg(moved(neg(s), d)), role, rot] = end[d] + L
                program.append(("send", d, role, rot, s))

    def ready_at(g, w):
        last = max(
            here.get((s, role, rot), 1e9)
            for s in ORDER[: LAST_SLOT[g] + 1]
            for role in "CMO"
            for rot in range(4)
        )
        return max(last, w_ready if w else 3.5)

    while any(todo.values()) or chunks:
        service(t)
        now = [c for c in chunks if ready_at(*c) <= t]
        if now:
            chunks.remove(now[0])
            for q in range(SPLIT):
                if q:
                    service(t)
                program.append(("step", *now[0], q))
                t += chunk / SPLIT
        else:
            later = [v for v in here.values() if t < v < 1e8]
            later += [e - horizon for e in end.values() if e - horizon > t]
            later += [v for v in (ready_at(*c) for c in chunks) if t < v < 1e8]
            t = min(later) + 0.01
    return program


def segments():
    have = {((0, 0), role, rot) for role in "CMO" for rot in range(4)}
    done, flags, told = [], set(), 0
    parts, ops = [], []
    ready_stats = []

    def need(s, role, rot):
        if (s, role, rot) not in have:
            have.add((s, role, rot))
            ops.append(("wait", s, role, rot))

    for op in plan():
        if op[0] == "send":
            need(op[4], op[2], op[3])
            ops.append(op)
        elif op[0] == "w":
            ops.append(op)
        else:
            _, g, w, h = op
            if h == 0:
                if "meta" not in flags:
                    flags.add("meta")
                    ops.append(("meta",))
                if w not in flags:
                    flags.add(w)
                    ops.append(("w_wait", w))
                for s in ORDER[: LAST_SLOT[g] + 1]:
                    for role in "CMO":
                        for rot in range(4):
                            need(s, role, rot)
                done.append((g, w))
            parts.append(ops)
            ops = ready_stats
            ready_stats = []
            if h == SPLIT - 1:
                both = [k for k in range(GROUPS) if (k, 0) in done and (k, 1) in done]
                while told < len(both) and both[told] == told:
                    ops.append(("merge", told))
                    lo = 8 * told
                    for k in range(16):
                        if 3 * k + 2 < lo + 8 and 3 * k + 2 >= lo:
                            ops.append(("stat", k))
                            ready_stats.append(("stat_send", k))
                    told += 1
    parts.append(ops)
    parts[-1] += ready_stats
    return done, parts


def rates():
    earlier = min(1.0 / K, math.sqrt(math.log(K) / (K * (STEP - 1))))
    current = min(1.0 / K, math.sqrt(math.log(K) / (K * STEP)))
    return earlier, current


def sum_lanes(v):
    return jnp.sum(v, axis=1, keepdims=True)


def pick(j, lo, hi, blocks, run):
    full = [k for k in range(lo, hi) if blocks[k]]
    if not full:
        return
    if hi - lo == 1:
        run(blocks[lo])
        return
    mid = (lo + hi) // 2
    pl.when(j < mid)(lambda: pick(j, lo, mid, blocks, run))
    pl.when(j >= mid)(lambda: pick(j, mid, hi, blocks, run))


def kernel(
    hid, wt, tgt, lab, psc, ppr, nxt,
    out_ref,
    hbuf, wbuf, acc, meta_out, meta_in, two, trow, cols, sbuf, merged, st_out, st_in, xs_out, xs_in, lo_out, lo_in,
    h_load, w_load, h_send, h_recv, w_send, w_recv, meta_send, meta_recv, st_send, st_recv, xs_send, xs_recv,
    lo_send, lo_recv,
):
    my, mz, mx, mc = (lax.axis_index(a) for a in ALL)
    par = lax.rem(mx, 2)

    def device(dy=0, dz=0, dx=0, dc=0):
        y, z, x = lax.rem(my + dy, N), lax.rem(mz + dz, N), lax.rem(mx + dx, N)
        return ((y * N + z) * N + x) * 2 + lax.rem(mc + dc, 2)

    toward = {
        "+y": device(dy=1), "-y": device(dy=N - 1), "+z": device(dz=1), "-z": device(dz=N - 1),
        "+x": device(dx=1), "-x": device(dx=N - 1),
    }

    def remote(src, dst, send, recv, to):
        return pltpu.make_async_remote_copy(
            src_ref=src, dst_ref=dst, send_sem=send, recv_sem=recv, device_id=to,
            device_id_type=pl.DeviceIdType.LOGICAL,
        )

    def wait_for(ref, sem):
        pltpu.make_async_copy(ref, ref, sem).wait()

    loads = []
    for rg in range(3):
        for kq in range(4):
            rows = pl.ds(pl.multiple_of(mc * HALF + rg * 32, 32), 32)
            loads.append(
                pltpu.make_async_copy(
                    hid.at[rows, pl.ds(kq * 1024, 1024)], hbuf.at[POS[0, 0] * 3 + rg, kq], h_load.at[rg * 4 + kq]
                )
            )
    for load in loads:
        load.start()
    own_w = pltpu.make_async_copy(wt, wbuf.at[0], w_load)
    own_w.start()

    barrier = pltpu.get_barrier_semaphore()
    plane = [(dy, dz, dc) for dy in range(N) for dz in range(N) for dc in range(2) if (dy, dz, dc) != (0, 0, 0)]
    for dy, dz, dc in plane:
        pl.semaphore_signal(barrier, inc=1, device_id=device(dy, dz, 0, dc), device_id_type=pl.DeviceIdType.LOGICAL)
    for dx in range(1, N):
        pl.semaphore_signal(barrier, inc=1, device_id=device(0, 0, dx), device_id_type=pl.DeviceIdType.LOGICAL)

    lane = lax.broadcasted_iota(jnp.int32, (8, 128), 1)
    two[...] = jnp.zeros_like(two)
    two[0:1, 0:192] = tgt[...]
    two[1:2, 0:192] = lab[...]
    both = two[...]
    first = jnp.where(lane < HALF, both[:, :128], -1).astype(F32)
    second = jnp.where(lane < HALF, pltpu.roll(both, 256 - HALF, 1)[:, :128], -1).astype(F32)
    meta_out[...] = jnp.zeros_like(meta_out)
    meta_out[0:1] = jnp.where(mc == 0, first[0:1], second[0:1])
    meta_out[1:2] = first[1:2]
    meta_out[2:3] = second[1:2]
    meta_out[3:4, 0:4] = psc[...]
    meta_out[4:5, 0:4] = ppr[...]
    meta_in[POS[0, 0]] = meta_out[...]
    for load in loads:
        load.wait()
    pl.semaphore_wait(barrier, len(plane) + N - 1)

    for s in ORDER[1:]:
        k = POS[neg(s)]
        remote(meta_out, meta_in.at[k], meta_send, meta_recv.at[k], device(s[0], s[1])).start()

    def piece(slot, role, rot):
        rg = {"C": 0, "M": 1 + par, "O": 2 - par}[role]
        return hbuf.at[slot * 3 + rg, rot], (slot * 3 + rg, rot)

    half_sub = lax.broadcasted_iota(jnp.int32, (K, 128), 0)
    half_lane = lax.broadcasted_iota(jnp.int32, (K, 128), 1)

    def do_meta():
        for k in range(1, 16):
            wait_for(meta_in.at[k], meta_recv.at[k])
        wide_lane = lax.broadcasted_iota(jnp.int32, (8, 256), 1)
        rows = [jnp.zeros((8, 256), F32) for _ in range(GROUPS)]
        counts = jnp.zeros((K, 128), F32)
        score = jnp.zeros((K, 128), F32)
        prob = jnp.zeros((K, 128), F32)
        for k, s in enumerate(ORDER):
            tile = meta_in[k]
            wide = jnp.concatenate([tile, tile], axis=1)
            at = 3 * k
            g, off = at // 8, 32 * (at % 8)
            n = min(3, 8 - at % 8)
            turned = pltpu.roll(wide, off, 1) if off else wide
            rows[g] = jnp.where((wide_lane >= off) & (wide_lane < off + 32 * n), turned, rows[g])
            if n < 3:
                turned = pltpu.roll(wide, 256 - 32 * n, 1)
                rows[g + 1] = jnp.where(wide_lane < 32 * (3 - n), turned, rows[g + 1])
            sub = half_sub.astype(F32)
            for r in (1, 2):
                counts += jnp.where(tile[r : r + 1] == sub, 1.0, 0.0)
            dp = lax.rem(my + s[0], N) * N + lax.rem(mz + s[1], N)
            mine = (half_lane == half_sub - 4 * dp) & (half_lane < 4)
            score += jnp.where(mine, tile[3:4], 0.0)
            prob += jnp.where(mine, tile[4:5], 0.0)
        for g in range(GROUPS):
            trow[g] = rows[g].astype(jnp.int32)
        for i, v in enumerate((counts, score, prob)):
            cols[i] = jnp.broadcast_to(sum_lanes(v), (K, 128))

    def joined(tiles):
        top = functools.reduce(jnp.maximum, [t[0:1] for t in tiles])
        total = functools.reduce(jnp.add, [t[1:2] * jnp.exp(t[0:1] - top) for t in tiles])
        return top, total, functools.reduce(jnp.add, [t[2:3] for t in tiles])

    def run(ops):
        for op in ops:
            if op[0] == "wait":
                _, s, role, rot = op
                ref, (i, r) = piece(POS[s], role, rot)
                wait_for(ref, h_recv.at[i, r])
            elif op[0] == "send":
                _, d, role, rot, s = op
                src, _ = piece(POS[s], role, rot)
                slot = POS[s] if d[1] == "x" else POS[neg(moved(neg(s), d))]
                dst, (i, r) = piece(slot, role, rot)
                remote(src, dst, h_send, h_recv.at[i, r], toward[d]).start()
            elif op[0] == "w":
                rows = pl.ds(op[1] * 128, min(128, COLS - op[1] * 128))
                remote(
                    wt.at[rows], wbuf.at[1, rows], w_send.at[op[1]], w_recv.at[op[1]], device(dc=1)
                ).start()
            elif op[0] == "w_wait":
                if op[1] == 0:
                    own_w.wait()
                else:
                    for i in range(N_W):
                        rows = pl.ds(i * 128, min(128, COLS - i * 128))
                        wait_for(wbuf.at[1, rows], w_recv.at[i])
            elif op[0] == "meta":
                do_meta()
            elif op[0] == "merge":
                for i, v in enumerate(joined([sbuf[op[1], q] for q in range(2)])):
                    merged[op[1], i : i + 1] = v
            elif op[0] == "stat":
                k = op[1]
                at = 3 * k
                g, off = at // 8, 32 * (at % 8)
                n = min(3, 8 - at % 8)
                tile = merged[g]
                msg = (pltpu.roll(tile, 256 - off, 1) if off else tile)[:, :128]
                if n < 3:
                    msg = jnp.where(lane < 32 * n, msg, pltpu.roll(merged[g + 1], 32 * n, 1)[:, :128])
                if opposite(ORDER[k]) == (0, 0):
                    st_in[0] = msg
                else:
                    st_out[k] = msg
            elif op[0] == "stat_send":
                k = op[1]
                s = opposite(ORDER[k])
                if s != (0, 0):
                    i = POS[neg(s)]
                    remote(st_out.at[k], st_in.at[i], st_send, st_recv.at[i], device(s[0], s[1])).start()

    base = ((my * N + mz) * 8 + mx * 2) * COLS
    chunks, parts = segments()
    run(parts[0])

    steps = [(g, w, q) for g, w in chunks for q in range(SPLIT)]

    def of(j, values):
        out = jnp.int32(values[0])
        for k in range(1, len(values)):
            if values[k] != values[k - 1]:
                out = jnp.where(j >= k, values[k], out)
        return out

    def step(j, _):
        pick(j, 0, len(steps), [[]] + parts[1:-1], run)
        g, w = (of(j, [c[i] for c in steps]) for i in range(2))
        q = lax.rem(j, SPLIT)
        per = 4 // SPLIT
        wide = WIDE // SPLIT
        rhs = jnp.concatenate(
            [hbuf[pl.ds(8 * g, 8), q * per + i].reshape(ROWS_G, 1024) for i in range(per)], axis=1
        )
        lhs = wbuf[w, :, pl.ds(pl.multiple_of(q * wide, wide), wide)]
        part = lax.dot_general(lhs, rhs, NT, preferred_element_type=F32)

        @pl.when(q == 0)
        def _():
            acc[...] = part

        @pl.when((q > 0) & (q < SPLIT - 1))
        def _():
            acc[...] += part

        @pl.when(q == SPLIT - 1)
        def _():
            logits = acc[...] + part
            row = lax.broadcasted_iota(jnp.int32, logits.shape, 0)
            target = trow[g][0:1] - (base + jnp.where(w == 0, mc, 1 - mc) * COLS)
            top = jnp.max(logits, axis=0, keepdims=True)
            sbuf[g, w, 0:1] = top
            sbuf[g, w, 1:2] = jnp.sum(jnp.exp(logits - top), axis=0, keepdims=True)
            sbuf[g, w, 2:3] = jnp.sum(jnp.where(row == target, logits, 0.0), axis=0, keepdims=True)

        return 0

    lax.fori_loop(0, len(steps), step, 0)
    run(parts[-1])

    for k in range(1, 16):
        wait_for(st_in.at[k], st_recv.at[k])

    for i, v in enumerate(joined([st_in[k] for k in range(16)])):
        xs_out[i : i + 1] = v
    for dx in range(1, N):
        remote(xs_out, xs_in.at[N - dx], xs_send, xs_recv.at[N - dx], device(dx=dx)).start()
    xs_in[0] = xs_out[...]
    for dx in range(1, N):
        wait_for(xs_in.at[dx], xs_recv.at[dx])
    top, total, picked = joined([xs_in[dx] for dx in range(N)])
    loss = top + jnp.log(total) - picked
    lo_out[...] = loss
    for dy, dz, dc in plane:
        i = POS[neg((dy, dz))] * 2 + dc
        remote(lo_out, lo_in.at[i], lo_send, lo_recv.at[i], device(dy, dz, 0, dc)).start()
    lo_in[0] = lo_out[...]
    for i in range(1, 32):
        wait_for(lo_in.at[i], lo_recv.at[i])

    sums = jnp.zeros((K, 128), F32)
    sub = half_sub.astype(F32)
    for k in range(16):
        tile = meta_in[POS[opposite(ORDER[k])]]
        for dc in range(2):
            labels = jnp.where(lax.rem(mc + dc, 2) == 0, tile[1:2], tile[2:3])
            sums += jnp.where(labels == sub, lo_in[2 * k + dc], 0.0)
    sums = jnp.broadcast_to(sum_lanes(sums), (K, 128))
    earlier, current = rates()
    score = current / earlier * cols[1] + current * (sums / cols[0]) / cols[2]
    weight = jnp.exp(score - jnp.max(score, axis=0, keepdims=True))
    probs = (1.0 - K * current) * (weight / jnp.sum(weight, axis=0, keepdims=True)) + current
    log_probs = jnp.log(probs)
    dp = my * N + mz

    def across(mask, v):
        return jnp.sum(jnp.where(mask, v, 0.0), axis=0, keepdims=True)

    out_ref[1:2] = across(half_lane == half_sub - 4 * dp, score)
    out_ref[2:3] = across(half_lane == half_sub, log_probs)
    two[2:3, 0:16] = nxt[...]
    chosen = across(two[2:3, :128] == half_sub, probs)
    out_ref[3:4] = 1.0 / (K * chosen)
    own = 2 * POS[2, 2]
    loss = jnp.where(mx // 2 == mc, lo_in[own], lo_in[own + 1])
    loss = jnp.broadcast_to(loss, (8, 128))
    out = loss
    for q in range(1, 4):
        out = jnp.where(2 * lax.rem(mx, 2) + mc == q, pltpu.roll(loss, 128 - 24 * q, 1), out)
    out_ref[0:1] = out[0:1]

    wait_for(hbuf.at[pl.ds(0, 45)], h_send)
    for i in range(N_W):
        rows = pl.ds(i * 128, min(128, COLS - i * 128))
        wait_for(wbuf.at[1, rows], w_send.at[i])
    wait_for(meta_in.at[pl.ds(0, 15)], meta_send)
    wait_for(st_in.at[pl.ds(0, 15)], st_send)
    wait_for(xs_in.at[pl.ds(0, 3)], xs_send)
    wait_for(lo_in.at[pl.ds(0, 31)], lo_send)


def finish(rows, *outs):
    for i, out in enumerate(outs):
        out[...] = rows[i : i + 1, : out.shape[1]]


def body(hidden, output_weight, targets, labels, prev_scores, prev_probs, next_domains):
    dma = pltpu.SemaphoreType.DMA
    vmem = pl.BlockSpec(memory_space=pltpu.VMEM)
    rows = pl.pallas_call(
        kernel,
        out_shape=jax.ShapeDtypeStruct((8, 128), F32),
        in_specs=[pl.BlockSpec(memory_space=pl.ANY)] * 2 + [vmem] * 5,
        out_specs=vmem,
        scratch_shapes=[
            pltpu.VMEM((48, 4, 32, 1024), jnp.bfloat16),
            pltpu.VMEM((2, COLS, WIDE), jnp.bfloat16),
            pltpu.VMEM((COLS, ROWS_G), F32),
            pltpu.VMEM((8, 128), F32),
            pltpu.VMEM((16, 8, 128), F32),
            pltpu.VMEM((8, 256), jnp.int32),
            pltpu.VMEM((GROUPS, 8, 256), jnp.int32),
            pltpu.VMEM((3, K, 128), F32),
            pltpu.VMEM((GROUPS, 2, 8, 256), F32),
            pltpu.VMEM((GROUPS, 8, 256), F32),
            pltpu.VMEM((16, 8, 128), F32),
            pltpu.VMEM((16, 8, 128), F32),
            pltpu.VMEM((8, 128), F32),
            pltpu.VMEM((N, 8, 128), F32),
            pltpu.VMEM((1, 128), F32),
            pltpu.VMEM((32, 1, 128), F32),
            dma((12,)),
            dma(()),
            dma(()),
            dma((48, 4)),
            dma((N_W,)),
            dma((N_W,)),
            dma(()),
            dma((16,)),
            dma(()),
            dma((16,)),
            dma(()),
            dma((N,)),
            dma(()),
            dma((32,)),
        ],
        compiler_params=pltpu.CompilerParams(
            collective_id=0, has_side_effects=True, vmem_limit_bytes=56 * 1024 * 1024
        ),
    )(
        hidden,
        output_weight.T,
        targets.reshape(1, -1),
        labels.reshape(1, -1),
        prev_scores.reshape(1, -1),
        prev_probs.reshape(1, -1),
        next_domains.reshape(1, -1),
    )
    sizes = (24, 4, K, 16)
    outs = pl.pallas_call(
        finish,
        out_shape=[jax.ShapeDtypeStruct((1, n), F32) for n in sizes],
        in_specs=[vmem],
        out_specs=[vmem] * 4,
    )(rows)
    return tuple(o.reshape(-1) for o in outs)


def solution(mesh):
    torus = Mesh(mesh.devices.reshape(N, N, N, 2), ALL)
    return jax.shard_map(
        body,
        mesh=torus,
        in_specs=(P(DP, None), P(None, ALL), P(DP), P(DP, None), P(DP), P(DP), P(DP)),
        out_specs=(P(ALL), P(DP), P(), P(DP)),
        check_vma=False,
    )
```

```python
import functools
import math

import jax
import jax.numpy as jnp
from jax import lax
from jax.experimental import pallas as pl
from jax.experimental.pallas import tpu as pltpu
from jax.sharding import Mesh
from jax.sharding import PartitionSpec as P

K = 64
STEP = 2000
N = 4
HALF = 96
COLS = 1002
WIDE = 4096
DP = ("y", "z")
TENSOR = ("x", "c")
ALL = ("y", "z", "x", "c")
DIRS = ("+y", "-y", "+z", "-z")
F32 = jnp.float32
NT = (((1,), (1,)), ((), ()))


ORDER = [
    (0, 0), (0, 1), (0, 3), (1, 0), (3, 0), (1, 3), (3, 1), (1, 1),
    (3, 3), (0, 2), (2, 0), (1, 2), (2, 1), (2, 3), (3, 2), (2, 2),
]
POS = {s: k for k, s in enumerate(ORDER)}
LAST_SLOT = [2, 5, 7, 10, 13, 15]
GROUPS = len(LAST_SLOT)
ROWS_G = 256
N_W = 8
FAR = (2, 2)
EARLY = 13


def group_of(slot):
    return next(g for g, k in enumerate(LAST_SLOT) if slot <= k)


def moved(n, d):
    k = 1 if d[0] == "+" else -1
    return ((n[0] + (k if d[1] == "y" else 0)) % N, (n[1] + (k if d[1] == "z" else 0)) % N)


def before(n, d):
    return moved(n, ("-" if d[0] == "+" else "+") + d[1])


def opposite(s):
    return ((s[0] + 2) % N, (s[1] + 2) % N)


def neg(n):
    return ((-n[0]) % N, (-n[1]) % N)


def children(rot, n):
    axis, sign = rot // 2, 1 - 2 * (rot % 2)
    a, b = n if axis == 0 else n[::-1]
    a, b = (a * sign) % N, (b * sign) % N
    first, second = ("y", "z") if axis == 0 else ("z", "y")
    fwd, back = ("+", "-") if sign == 1 else ("-", "+")
    out = []
    if b == 0:
        if a in (0, 1):
            out.append(fwd + first)
        if a == 0:
            out.append(back + first)
    if b in (0, 1):
        out.append(fwd + second)
    if b == 0:
        out.append(back + second)
    return out


def x_dir(rot):
    return "+x" if rot % 2 == 0 else "-x"


def columns_of(role, rot):
    return rot if role == "C" else (rot + 2) % 4


def wanted(role, rot, n, step, lead):
    return step * (group_of(POS[neg(n)]) + 1) - (lead if columns_of(role, rot) < 2 else 0.0)


def due(role, rot, n, hop, step, lead):
    out = wanted(role, rot, n, step, lead)
    for d in children(rot, n):
        out = min(out, due(role, rot, moved(n, d), hop, step, lead) - hop)
    if role == "M" and n not in ((0, 0), FAR):
        out = min(out, wanted("O", rot, n, step, lead) - hop)
    return out


def plan(T=1.45, L=2.7, hop=4.5, step=3.0, lead=2.0, chunk=3.6, horizon=2.2, w_ready=15.0, t0=1.2):
    here = {((0, 0), role, rot): 0.0 for role in "CMO" for rot in range(4)}
    todo = {d: [] for d in DIRS + ("+x", "-x")}
    for role in "CM":
        for rot in range(4):
            for n in ORDER:
                for d in children(rot, n):
                    todo[d].append((due(role, rot, moved(n, d), hop, step, lead), neg(n), role, rot))
                if role == "M" and n not in ((0, 0), FAR):
                    late = wanted("O", rot, n, step, lead)
                    todo[x_dir(rot)].append((late, neg(n), role, rot))
    for rot, d in enumerate(DIRS):
        todo[d].append((wanted("O", rot, FAR, step, lead), neg(before(FAR, d)), "O", rot))
    end = {d: 0.0 for d in todo}
    chunks = [(g, w, q) for g in range(GROUPS) for q in range(2) for w in range(2)]
    program, t, w_sent = [], t0, 0

    def service(t):
        nonlocal w_sent
        if w_sent < N_W:
            program.append(("w", w_sent))
            w_sent += 1
        for d in todo:
            while end[d] < t + horizon:
                ready = [
                    (late, here[s, role, rot], s, role, rot)
                    for late, s, role, rot in todo[d]
                    if here.get((s, role, rot), 1e9) <= t
                ]
                if not ready:
                    break
                late, _, s, role, rot = min(ready)
                todo[d].remove((late, s, role, rot))
                end[d] = max(t + 0.05, end[d]) + T
                if d[1] == "x":
                    here[s, "O", rot] = end[d] + L
                else:
                    here[neg(moved(neg(s), d)), role, rot] = end[d] + L
                program.append(("send", d, role, rot, s))

    def ready_at(g, w, q):
        last = max(
            here.get((s, role, rot), 1e9)
            for s in ORDER[: LAST_SLOT[g] + 1]
            for role in "CMO"
            for rot in range(4)
            if columns_of(role, rot) // 2 == q
        )
        return max(last, w_ready if w else 3.5)

    def free(g, w, q):
        return ((g, w, 0) if q else (g - 2, w, 1)) not in chunks

    while any(todo.values()) or chunks:
        service(t)
        now = [c for c in chunks if ready_at(*c) <= t and free(*c)]
        if now:
            chunks.remove(now[0])
            program.append(("step", *now[0]))
            t += chunk / 2
        else:
            later = [v for v in here.values() if t < v < 1e8]
            later += [e - horizon for e in end.values() if e - horizon > t]
            later += [v for v in (ready_at(*c) for c in chunks) if t < v < 1e8]
            t = min(later) + 0.01
    return program


def segments():
    have = {((0, 0), role, rot) for role in "CMO" for rot in range(4)}
    done, flags, told = [], set(), 0
    parts, ops = [], []
    ready_stats = []

    def need(s, role, rot):
        if (s, role, rot) not in have:
            have.add((s, role, rot))
            ops.append(("wait", s, role, rot))

    for op in plan():
        if op[0] == "send":
            need(op[4], op[2], op[3])
            ops.append(op)
        elif op[0] == "w":
            ops.append(op)
        else:
            _, g, w, q = op
            if "meta" not in flags:
                flags.add("meta")
                ops.append(("meta",))
            if w not in flags:
                flags.add(w)
                ops.append(("w_wait", w))
            for s in ORDER[: LAST_SLOT[g] + 1]:
                for role in "CMO":
                    for rot in range(4):
                        if columns_of(role, rot) // 2 == q:
                            need(s, role, rot)
            done.append((g, w, q))
            parts.append(ops)
            ops = ready_stats
            ready_stats = []
            if q == 1:
                both = [k for k in range(GROUPS) if (k, 0, 1) in done and (k, 1, 1) in done]
                while told < len(both) and both[told] == told:
                    ops.append(("merge", told))
                    lo = 8 * told
                    for k in range(16):
                        if 3 * k + 2 < lo + 8 and 3 * k + 2 >= lo:
                            ops.append(("stat", k))
                            ready_stats.append(("stat_send", k))
                    told += 1
    parts.append(ops)
    parts[-1] += ready_stats
    assert any(("stat_send", EARLY - 1) in p for p in parts[:-1])
    parts[-2] = parts[-2] + [("early",)]
    return done, parts


def rates():
    earlier = min(1.0 / K, math.sqrt(math.log(K) / (K * (STEP - 1))))
    current = min(1.0 / K, math.sqrt(math.log(K) / (K * STEP)))
    return earlier, current


def sum_lanes(v):
    return jnp.sum(v, axis=1, keepdims=True)


def pick(j, lo, hi, blocks, run):
    full = [k for k in range(lo, hi) if blocks[k]]
    if not full:
        return
    if hi - lo == 1:
        run(blocks[lo])
        return
    mid = (lo + hi) // 2
    pl.when(j < mid)(lambda: pick(j, lo, mid, blocks, run))
    pl.when(j >= mid)(lambda: pick(j, mid, hi, blocks, run))


def kernel(
    hid, wt, tgt, lab, psc, ppr, nxt,
    out_ref,
    hbuf, wbuf, acc, meta_out, meta_in, two, trow, cols, sbuf, merged, st_out, st_in, lt_in, xs_out, xs_in, lo_out, lo_in,
    h_load, w_load, h_send, h_recv, w_send, w_recv, meta_send, meta_recv, st_send, st_recv, lt_send, lt_recv, xs_send, xs_recv,
    lo_send, lo_recv,
):
    my, mz, mx, mc = (lax.axis_index(a) for a in ALL)
    par = lax.rem(mx, 2)

    def device(dy=0, dz=0, dx=0, dc=0):
        y, z, x = lax.rem(my + dy, N), lax.rem(mz + dz, N), lax.rem(mx + dx, N)
        return ((y * N + z) * N + x) * 2 + lax.rem(mc + dc, 2)

    toward = {
        "+y": device(dy=1), "-y": device(dy=N - 1), "+z": device(dz=1), "-z": device(dz=N - 1),
        "+x": device(dx=1), "-x": device(dx=N - 1),
    }

    def remote(src, dst, send, recv, to):
        return pltpu.make_async_remote_copy(
            src_ref=src, dst_ref=dst, send_sem=send, recv_sem=recv, device_id=to,
            device_id_type=pl.DeviceIdType.LOGICAL,
        )

    def wait_for(ref, sem):
        pltpu.make_async_copy(ref, ref, sem).wait()

    loads = []
    for rg in range(3):
        for kq in range(4):
            rows = pl.ds(pl.multiple_of(mc * HALF + rg * 32, 32), 32)
            loads.append(
                pltpu.make_async_copy(
                    hid.at[rows, pl.ds(kq * 1024, 1024)], hbuf.at[POS[0, 0] * 3 + rg, kq], h_load.at[rg * 4 + kq]
                )
            )
    for load in loads:
        load.start()
    own_w = pltpu.make_async_copy(wt, wbuf.at[0], w_load)
    own_w.start()

    barrier = pltpu.get_barrier_semaphore()
    plane = [(dy, dz, dc) for dy in range(N) for dz in range(N) for dc in range(2) if (dy, dz, dc) != (0, 0, 0)]
    for dy, dz, dc in plane:
        pl.semaphore_signal(barrier, inc=1, device_id=device(dy, dz, 0, dc), device_id_type=pl.DeviceIdType.LOGICAL)
    beside = [(dy, dz, dx) for dy, dz in ((0, 0), (0, 1), (0, 3), (1, 0), (3, 0)) for dx in range(1, N)]
    for dy, dz, dx in beside:
        pl.semaphore_signal(barrier, inc=1, device_id=device(dy, dz, dx), device_id_type=pl.DeviceIdType.LOGICAL)

    lane = lax.broadcasted_iota(jnp.int32, (8, 128), 1)
    two[...] = jnp.zeros_like(two)
    two[0:1, 0:192] = tgt[...]
    two[1:2, 0:192] = lab[...]
    both = two[...]
    first = jnp.where(lane < HALF, both[:, :128], -1).astype(F32)
    second = jnp.where(lane < HALF, pltpu.roll(both, 256 - HALF, 1)[:, :128], -1).astype(F32)
    meta_out[...] = jnp.zeros_like(meta_out)
    meta_out[0:1] = jnp.where(mc == 0, first[0:1], second[0:1])
    meta_out[1:2] = first[1:2]
    meta_out[2:3] = second[1:2]
    meta_out[3:4, 0:4] = psc[...]
    meta_out[4:5, 0:4] = ppr[...]
    meta_in[POS[0, 0]] = meta_out[...]
    for load in loads:
        load.wait()
    pl.semaphore_wait(barrier, len(plane) + len(beside))

    for s in ORDER[1:]:
        k = POS[neg(s)]
        remote(meta_out, meta_in.at[k], meta_send, meta_recv.at[k], device(s[0], s[1])).start()

    def piece(slot, role, rot):
        i = slot * 3 + {"C": 0, "M": 1 + par, "O": 2 - par}[role], columns_of(role, rot)
        return hbuf.at[i], i

    half_sub = lax.broadcasted_iota(jnp.int32, (K, 128), 0)
    half_lane = lax.broadcasted_iota(jnp.int32, (K, 128), 1)

    def do_meta():
        for k in range(1, 16):
            wait_for(meta_in.at[k], meta_recv.at[k])
        wide_lane = lax.broadcasted_iota(jnp.int32, (8, 256), 1)
        rows = [jnp.zeros((8, 256), F32) for _ in range(GROUPS)]
        counts = jnp.zeros((K, 128), F32)
        score = jnp.zeros((K, 128), F32)
        prob = jnp.zeros((K, 128), F32)
        for k, s in enumerate(ORDER):
            tile = meta_in[k]
            wide = jnp.concatenate([tile, tile], axis=1)
            at = 3 * k
            g, off = at // 8, 32 * (at % 8)
            n = min(3, 8 - at % 8)
            turned = pltpu.roll(wide, off, 1) if off else wide
            rows[g] = jnp.where((wide_lane >= off) & (wide_lane < off + 32 * n), turned, rows[g])
            if n < 3:
                turned = pltpu.roll(wide, 256 - 32 * n, 1)
                rows[g + 1] = jnp.where(wide_lane < 32 * (3 - n), turned, rows[g + 1])
            sub = half_sub.astype(F32)
            for r in (1, 2):
                counts += jnp.where(tile[r : r + 1] == sub, 1.0, 0.0)
            dp = lax.rem(my + s[0], N) * N + lax.rem(mz + s[1], N)
            mine = (half_lane == half_sub - 4 * dp) & (half_lane < 4)
            score += jnp.where(mine, tile[3:4], 0.0)
            prob += jnp.where(mine, tile[4:5], 0.0)
        for g in range(GROUPS):
            trow[g] = rows[g].astype(jnp.int32)
        for i, v in enumerate((counts, score, prob)):
            cols[i] = jnp.broadcast_to(sum_lanes(v), (K, 128))

    def joined(tiles):
        top = functools.reduce(jnp.maximum, [t[0:1] for t in tiles])
        total = functools.reduce(jnp.add, [t[1:2] * jnp.exp(t[0:1] - top) for t in tiles])
        return top, total, functools.reduce(jnp.add, [t[2:3] for t in tiles])

    def run(ops):
        for op in ops:
            if op[0] == "wait":
                _, s, role, rot = op
                ref, (i, r) = piece(POS[s], role, rot)
                wait_for(ref, h_recv.at[i, r])
            elif op[0] == "send":
                _, d, role, rot, s = op
                src, _ = piece(POS[s], role, rot)
                slot = POS[s] if d[1] == "x" else POS[neg(moved(neg(s), d))]
                dst, (i, r) = piece(slot, role, rot)
                remote(src, dst, h_send, h_recv.at[i, r], toward[d]).start()
            elif op[0] == "w":
                rows = pl.ds(op[1] * 128, min(128, COLS - op[1] * 128))
                remote(
                    wt.at[rows], wbuf.at[1, rows], w_send.at[op[1]], w_recv.at[op[1]], device(dc=1)
                ).start()
            elif op[0] == "w_wait":
                if op[1] == 0:
                    own_w.wait()
                else:
                    for i in range(N_W):
                        rows = pl.ds(i * 128, min(128, COLS - i * 128))
                        wait_for(wbuf.at[1, rows], w_recv.at[i])
            elif op[0] == "meta":
                do_meta()
            elif op[0] == "merge":
                for i, v in enumerate(joined([sbuf[op[1], q] for q in range(2)])):
                    merged[op[1], i : i + 1] = v
            elif op[0] == "stat":
                k = op[1]
                at = 3 * k
                g, off = at // 8, 32 * (at % 8)
                n = min(3, 8 - at % 8)
                tile = merged[g]
                msg = (pltpu.roll(tile, 256 - off, 1) if off else tile)[:, :128]
                if n < 3:
                    msg = jnp.where(lane < 32 * n, msg, pltpu.roll(merged[g + 1], 32 * n, 1)[:, :128])
                st_out[k] = msg
                if ORDER[k] == FAR:
                    lt_in[k - EARLY, 0] = msg
            elif op[0] == "stat_send":
                k = op[1]
                s = opposite(ORDER[k])
                if k < EARLY:
                    remote(st_out.at[k], st_in.at[k], st_send, st_recv.at[k], device(s[0], s[1])).start()
                else:
                    for dx in range(N):
                        if s != (0, 0) or dx:
                            i = (k - EARLY, (N - dx) % N)
                            remote(
                                st_out.at[k], lt_in.at[i], lt_send, lt_recv.at[i], device(s[0], s[1], dx)
                            ).start()
            elif op[0] == "early":
                for k in range(EARLY):
                    wait_for(st_in.at[k], st_recv.at[k])
                for i, v in enumerate(joined([st_in[k] for k in range(EARLY)])):
                    xs_out[i : i + 1] = v
                xs_in[0] = xs_out[...]
                for dx in range(1, N):
                    remote(xs_out, xs_in.at[N - dx], xs_send, xs_recv.at[N - dx], device(dx=dx)).start()

    base = ((my * N + mz) * 8 + mx * 2) * COLS
    chunks, parts = segments()
    run(parts[0])

    steps = chunks

    def of(j, values):
        out = jnp.int32(values[0])
        for k in range(1, len(values)):
            if values[k] != values[k - 1]:
                out = jnp.where(j >= k, values[k], out)
        return out

    def step(j, _):
        pick(j, 0, len(steps), [[]] + parts[1:-1], run)
        g, w, q = (of(j, [c[i] for c in steps]) for i in range(3))
        per = 2
        wide = WIDE // 2
        rhs = jnp.concatenate(
            [hbuf[pl.ds(8 * g, 8), q * per + i].reshape(ROWS_G, 1024) for i in range(per)], axis=1
        )
        lhs = wbuf[w, :, pl.ds(pl.multiple_of(q * wide, wide), wide)]
        part = lax.dot_general(lhs, rhs, NT, preferred_element_type=F32)

        @pl.when(q == 0)
        def _():
            acc[lax.rem(g, 2), w] = part

        @pl.when(q == 1)
        def _():
            logits = acc[lax.rem(g, 2), w] + part
            row = lax.broadcasted_iota(jnp.int32, logits.shape, 0)
            target = trow[g][0:1] - (base + jnp.where(w == 0, mc, 1 - mc) * COLS)
            top = jnp.max(logits, axis=0, keepdims=True)
            sbuf[g, w, 0:1] = top
            sbuf[g, w, 1:2] = jnp.sum(jnp.exp(logits - top), axis=0, keepdims=True)
            sbuf[g, w, 2:3] = jnp.sum(jnp.where(row == target, logits, 0.0), axis=0, keepdims=True)

        return 0

    lax.fori_loop(0, len(steps), step, 0)
    run(parts[-1])

    late = [(k, dx) for k in range(16 - EARLY) for dx in range(N)]
    for k, dx in late:
        if ORDER[EARLY + k] != FAR or dx:
            wait_for(lt_in.at[k, dx], lt_recv.at[k, dx])
    for dx in range(1, N):
        wait_for(xs_in.at[dx], xs_recv.at[dx])
    top, total, picked = joined([xs_in[dx] for dx in range(N)] + [lt_in[k, dx] for k, dx in late])
    loss = top + jnp.log(total) - picked
    lo_out[...] = loss
    for dy, dz, dc in plane:
        i = POS[neg((dy, dz))] * 2 + dc
        remote(lo_out, lo_in.at[i], lo_send, lo_recv.at[i], device(dy, dz, 0, dc)).start()
    lo_in[0] = lo_out[...]
    for i in range(1, 32):
        wait_for(lo_in.at[i], lo_recv.at[i])

    sums = jnp.zeros((K, 128), F32)
    sub = half_sub.astype(F32)
    for k in range(16):
        tile = meta_in[POS[opposite(ORDER[k])]]
        for dc in range(2):
            labels = jnp.where(lax.rem(mc + dc, 2) == 0, tile[1:2], tile[2:3])
            sums += jnp.where(labels == sub, lo_in[2 * k + dc], 0.0)
    sums = jnp.broadcast_to(sum_lanes(sums), (K, 128))
    earlier, current = rates()
    score = current / earlier * cols[1] + current * (sums / cols[0]) / cols[2]
    weight = jnp.exp(score - jnp.max(score, axis=0, keepdims=True))
    probs = (1.0 - K * current) * (weight / jnp.sum(weight, axis=0, keepdims=True)) + current
    log_probs = jnp.log(probs)
    dp = my * N + mz

    def across(mask, v):
        return jnp.sum(jnp.where(mask, v, 0.0), axis=0, keepdims=True)

    out_ref[1:2] = across(half_lane == half_sub - 4 * dp, score)
    out_ref[2:3] = across(half_lane == half_sub, log_probs)
    two[2:3, 0:16] = nxt[...]
    chosen = across(two[2:3, :128] == half_sub, probs)
    out_ref[3:4] = 1.0 / (K * chosen)
    own = 2 * POS[2, 2]
    loss = jnp.where(mx // 2 == mc, lo_in[own], lo_in[own + 1])
    loss = jnp.broadcast_to(loss, (8, 128))
    out = loss
    for q in range(1, 4):
        out = jnp.where(2 * lax.rem(mx, 2) + mc == q, pltpu.roll(loss, 128 - 24 * q, 1), out)
    out_ref[0:1] = out[0:1]

    wait_for(hbuf.at[pl.ds(0, 45)], h_send)
    for i in range(N_W):
        rows = pl.ds(i * 128, min(128, COLS - i * 128))
        wait_for(wbuf.at[1, rows], w_send.at[i])
    wait_for(meta_in.at[pl.ds(0, 15)], meta_send)
    wait_for(st_in.at[pl.ds(0, EARLY)], st_send)
    wait_for(st_in.at[pl.ds(0, 11)], lt_send)
    wait_for(xs_in.at[pl.ds(0, 3)], xs_send)
    wait_for(lo_in.at[pl.ds(0, 31)], lo_send)


def finish(rows, *outs):
    for i, out in enumerate(outs):
        out[...] = rows[i : i + 1, : out.shape[1]]


def body(hidden, output_weight, targets, labels, prev_scores, prev_probs, next_domains):
    dma = pltpu.SemaphoreType.DMA
    vmem = pl.BlockSpec(memory_space=pltpu.VMEM)
    rows = pl.pallas_call(
        kernel,
        out_shape=jax.ShapeDtypeStruct((8, 128), F32),
        in_specs=[pl.BlockSpec(memory_space=pl.ANY)] * 2 + [vmem] * 5,
        out_specs=vmem,
        scratch_shapes=[
            pltpu.VMEM((48, 4, 32, 1024), jnp.bfloat16),
            pltpu.VMEM((2, COLS, WIDE), jnp.bfloat16),
            pltpu.VMEM((2, 2, COLS, ROWS_G), F32),
            pltpu.VMEM((8, 128), F32),
            pltpu.VMEM((16, 8, 128), F32),
            pltpu.VMEM((8, 256), jnp.int32),
            pltpu.VMEM((GROUPS, 8, 256), jnp.int32),
            pltpu.VMEM((3, K, 128), F32),
            pltpu.VMEM((GROUPS, 2, 8, 256), F32),
            pltpu.VMEM((GROUPS, 8, 256), F32),
            pltpu.VMEM((16, 8, 128), F32),
            pltpu.VMEM((16, 8, 128), F32),
            pltpu.VMEM((16 - EARLY, N, 8, 128), F32),
            pltpu.VMEM((8, 128), F32),
            pltpu.VMEM((N, 8, 128), F32),
            pltpu.VMEM((1, 128), F32),
            pltpu.VMEM((32, 1, 128), F32),
            dma((12,)),
            dma(()),
            dma(()),
            dma((48, 4)),
            dma((N_W,)),
            dma((N_W,)),
            dma(()),
            dma((16,)),
            dma(()),
            dma((16,)),
            dma(()),
            dma((16 - EARLY, N)),
            dma(()),
            dma((N,)),
            dma(()),
            dma((32,)),
        ],
        compiler_params=pltpu.CompilerParams(
            collective_id=0, has_side_effects=True, vmem_limit_bytes=56 * 1024 * 1024
        ),
    )(
        hidden,
        output_weight.T,
        targets.reshape(1, -1),
        labels.reshape(1, -1),
        prev_scores.reshape(1, -1),
        prev_probs.reshape(1, -1),
        next_domains.reshape(1, -1),
    )
    sizes = (24, 4, K, 16)
    outs = pl.pallas_call(
        finish,
        out_shape=[jax.ShapeDtypeStruct((1, n), F32) for n in sizes],
        in_specs=[vmem],
        out_specs=[vmem] * 4,
    )(rows)
    return tuple(o.reshape(-1) for o in outs)


def solution(mesh):
    torus = Mesh(mesh.devices.reshape(N, N, N, 2), ALL)
    return jax.shard_map(
        body,
        mesh=torus,
        in_specs=(P(DP, None), P(None, ALL), P(DP), P(DP, None), P(DP), P(DP), P(DP)),
        out_specs=(P(ALL), P(DP), P(), P(DP)),
        check_vma=False,
    )
```

```python
import functools
import math

import jax
import jax.numpy as jnp
from jax import lax
from jax.experimental import pallas as pl
from jax.experimental.pallas import tpu as pltpu
from jax.sharding import Mesh
from jax.sharding import PartitionSpec as P

K = 64
STEP = 2000
N = 4
HALF = 96
COLS = 1002
WIDE = 4096
DP = ("y", "z")
TENSOR = ("x", "c")
ALL = ("y", "z", "x", "c")
DIRS = ("+y", "-y", "+z", "-z")
F32 = jnp.float32
NT = (((1,), (1,)), ((), ()))


ORDER = [
    (0, 0), (0, 1), (0, 3), (1, 0), (3, 0), (1, 3), (3, 1), (1, 1),
    (3, 3), (0, 2), (2, 0), (1, 2), (2, 1), (2, 3), (3, 2), (2, 2),
]
POS = {s: k for k, s in enumerate(ORDER)}
LAST_SLOT = [2, 5, 7, 10, 13, 15]
GROUPS = len(LAST_SLOT)
ROWS_G = 256
N_W = 8
FAR = (2, 2)
EARLY = 13


def group_of(slot):
    return next(g for g, k in enumerate(LAST_SLOT) if slot <= k)


def moved(n, d):
    k = 1 if d[0] == "+" else -1
    return ((n[0] + (k if d[1] == "y" else 0)) % N, (n[1] + (k if d[1] == "z" else 0)) % N)


def before(n, d):
    return moved(n, ("-" if d[0] == "+" else "+") + d[1])


def opposite(s):
    return ((s[0] + 2) % N, (s[1] + 2) % N)


def hops(*offsets):
    return sum(min(k, N - k) for k in offsets)


def neg(n):
    return ((-n[0]) % N, (-n[1]) % N)


def children(rot, n):
    axis, sign = rot // 2, 1 - 2 * (rot % 2)
    a, b = n if axis == 0 else n[::-1]
    a, b = (a * sign) % N, (b * sign) % N
    first, second = ("y", "z") if axis == 0 else ("z", "y")
    fwd, back = ("+", "-") if sign == 1 else ("-", "+")
    out = []
    if b == 0:
        if a in (0, 1):
            out.append(fwd + first)
        if a == 0:
            out.append(back + first)
    if b in (0, 1):
        out.append(fwd + second)
    if b == 0:
        out.append(back + second)
    return out


def x_dir(rot):
    return "+x" if rot % 2 == 0 else "-x"


def columns_of(role, rot):
    return rot if role == "C" else (rot + 2) % 4


def wanted(role, rot, n, step, lead):
    return step * (group_of(POS[neg(n)]) + 1) - (lead if columns_of(role, rot) < 2 else 0.0)


def due(role, rot, n, hop, step, lead):
    out = wanted(role, rot, n, step, lead)
    for d in children(rot, n):
        out = min(out, due(role, rot, moved(n, d), hop, step, lead) - hop)
    if role == "M" and n not in ((0, 0), FAR):
        out = min(out, wanted("O", rot, n, step, lead) - hop)
    return out


def plan(T=1.45, L=2.7, hop=4.5, step=3.0, lead=2.0, chunk=3.6, horizon=2.2, w_ready=15.0, t0=1.2):
    here = {((0, 0), role, rot): 0.0 for role in "CMO" for rot in range(4)}
    todo = {d: [] for d in DIRS + ("+x", "-x")}
    for role in "CM":
        for rot in range(4):
            for n in ORDER:
                for d in children(rot, n):
                    todo[d].append((due(role, rot, moved(n, d), hop, step, lead), neg(n), role, rot))
                if role == "M" and n not in ((0, 0), FAR):
                    late = wanted("O", rot, n, step, lead)
                    todo[x_dir(rot)].append((late, neg(n), role, rot))
    for rot, d in enumerate(DIRS):
        todo[d].append((wanted("O", rot, FAR, step, lead), neg(before(FAR, d)), "O", rot))
    end = {d: 0.0 for d in todo}
    chunks = [(g, w, q) for g in range(GROUPS) for q in range(2) for w in range(2)]
    program, t, w_sent = [], t0, 0

    def service(t):
        nonlocal w_sent
        if w_sent < N_W:
            program.append(("w", w_sent))
            w_sent += 1
        for d in todo:
            while end[d] < t + horizon:
                ready = [
                    (late, here[s, role, rot], s, role, rot)
                    for late, s, role, rot in todo[d]
                    if here.get((s, role, rot), 1e9) <= t
                ]
                if not ready:
                    break
                late, _, s, role, rot = min(ready)
                todo[d].remove((late, s, role, rot))
                end[d] = max(t + 0.05, end[d]) + T
                if d[1] == "x":
                    here[s, "O", rot] = end[d] + L
                else:
                    here[neg(moved(neg(s), d)), role, rot] = end[d] + L
                program.append(("send", d, role, rot, s))

    def ready_at(g, w, q):
        last = max(
            here.get((s, role, rot), 1e9)
            for s in ORDER[: LAST_SLOT[g] + 1]
            for role in "CMO"
            for rot in range(4)
            if columns_of(role, rot) // 2 == q
        )
        return max(last, w_ready if w else 3.5)

    def free(g, w, q):
        return ((g, w, 0) if q else (g - 2, w, 1)) not in chunks

    while any(todo.values()) or chunks:
        service(t)
        now = [c for c in chunks if ready_at(*c) <= t and free(*c)]
        if now:
            chunks.remove(now[0])
            program.append(("step", *now[0]))
            t += chunk / 2
        else:
            later = [v for v in here.values() if t < v < 1e8]
            later += [e - horizon for e in end.values() if e - horizon > t]
            later += [v for v in (ready_at(*c) for c in chunks) if t < v < 1e8]
            t = min(later) + 0.01
    return program


def segments():
    have = {((0, 0), role, rot) for role in "CMO" for rot in range(4)}
    done, flags, told = [], set(), 0
    parts, ops = [], []
    ready_stats = []

    def need(s, role, rot):
        if (s, role, rot) not in have:
            have.add((s, role, rot))
            ops.append(("wait", s, role, rot))

    for op in plan():
        if op[0] == "send":
            need(op[4], op[2], op[3])
            ops.append(op)
        elif op[0] == "w":
            ops.append(op)
        else:
            _, g, w, q = op
            if "meta" not in flags:
                flags.add("meta")
                ops.append(("meta",))
            if w not in flags:
                flags.add(w)
                ops.append(("w_wait", w))
            for s in ORDER[: LAST_SLOT[g] + 1]:
                for role in "CMO":
                    for rot in range(4):
                        if columns_of(role, rot) // 2 == q:
                            need(s, role, rot)
            done.append((g, w, q))
            parts.append(ops)
            ops = ready_stats
            ready_stats = []
            if q == 1:
                both = [k for k in range(GROUPS) if (k, 0, 1) in done and (k, 1, 1) in done]
                while told < len(both) and both[told] == told:
                    ops.append(("merge", told))
                    lo = 8 * told
                    for k in range(16):
                        if 3 * k + 2 < lo + 8 and 3 * k + 2 >= lo:
                            ops.append(("stat", k))
                            ready_stats.append(("stat_send", k))
                    told += 1
    parts.append(ops)
    parts[-1] += ready_stats
    assert any(("stat_send", EARLY - 1) in p for p in parts[:-1])
    parts[-2] = parts[-2] + [("early",)]
    return done, parts


def rates():
    earlier = min(1.0 / K, math.sqrt(math.log(K) / (K * (STEP - 1))))
    current = min(1.0 / K, math.sqrt(math.log(K) / (K * STEP)))
    return earlier, current


def sum_lanes(v):
    return jnp.sum(v, axis=1, keepdims=True)


def pick(j, lo, hi, blocks, run):
    full = [k for k in range(lo, hi) if blocks[k]]
    if not full:
        return
    if hi - lo == 1:
        run(blocks[lo])
        return
    mid = (lo + hi) // 2
    pl.when(j < mid)(lambda: pick(j, lo, mid, blocks, run))
    pl.when(j >= mid)(lambda: pick(j, mid, hi, blocks, run))


def kernel(
    hid, wt, tgt, lab, psc, ppr, nxt,
    out_ref,
    hbuf, wbuf, acc, meta_out, meta_in, two, trow, cols, sbuf, merged, st_out, st_in, lt_in, xs_out, xs_in, lo_out, lo_in,
    h_load, w_load, h_send, h_recv, w_send, w_recv, meta_send, meta_recv, st_send, st_recv, lt_send, lt_recv, xs_send, xs_recv,
    lo_send, lo_recv,
):
    my, mz, mx, mc = (lax.axis_index(a) for a in ALL)
    par = lax.rem(mx, 2)

    def device(dy=0, dz=0, dx=0, dc=0):
        y, z, x = lax.rem(my + dy, N), lax.rem(mz + dz, N), lax.rem(mx + dx, N)
        return ((y * N + z) * N + x) * 2 + lax.rem(mc + dc, 2)

    toward = {
        "+y": device(dy=1), "-y": device(dy=N - 1), "+z": device(dz=1), "-z": device(dz=N - 1),
        "+x": device(dx=1), "-x": device(dx=N - 1),
    }

    def remote(src, dst, send, recv, to):
        return pltpu.make_async_remote_copy(
            src_ref=src, dst_ref=dst, send_sem=send, recv_sem=recv, device_id=to,
            device_id_type=pl.DeviceIdType.LOGICAL,
        )

    def wait_for(ref, sem):
        pltpu.make_async_copy(ref, ref, sem).wait()

    loads = []
    for rg in range(3):
        for kq in range(4):
            rows = pl.ds(pl.multiple_of(mc * HALF + rg * 32, 32), 32)
            loads.append(
                pltpu.make_async_copy(
                    hid.at[rows, pl.ds(kq * 1024, 1024)], hbuf.at[POS[0, 0] * 3 + rg, kq], h_load.at[rg * 4 + kq]
                )
            )
    for load in loads:
        load.start()
    own_w = pltpu.make_async_copy(wt, wbuf.at[0], w_load)
    own_w.start()

    barrier = pltpu.get_barrier_semaphore()
    plane = [(dy, dz, dc) for dy in range(N) for dz in range(N) for dc in range(2) if (dy, dz, dc) != (0, 0, 0)]
    plane.sort(key=lambda p: -hops(*p))
    for dy, dz, dc in plane:
        pl.semaphore_signal(barrier, inc=1, device_id=device(dy, dz, 0, dc), device_id_type=pl.DeviceIdType.LOGICAL)
    beside = [(dy, dz, dx) for dy, dz in ((0, 0), (0, 1), (0, 3), (1, 0), (3, 0)) for dx in range(1, N)]
    beside.sort(key=lambda p: -hops(*p))
    for dy, dz, dx in beside:
        pl.semaphore_signal(barrier, inc=1, device_id=device(dy, dz, dx), device_id_type=pl.DeviceIdType.LOGICAL)

    lane = lax.broadcasted_iota(jnp.int32, (8, 128), 1)
    two[...] = jnp.zeros_like(two)
    two[0:1, 0:192] = tgt[...]
    two[1:2, 0:192] = lab[...]
    both = two[...]
    first = jnp.where(lane < HALF, both[:, :128], -1).astype(F32)
    second = jnp.where(lane < HALF, pltpu.roll(both, 256 - HALF, 1)[:, :128], -1).astype(F32)
    meta_out[...] = jnp.zeros_like(meta_out)
    meta_out[0:1] = jnp.where(mc == 0, first[0:1], second[0:1])
    meta_out[1:2] = first[1:2]
    meta_out[2:3] = second[1:2]
    meta_out[3:4, 0:4] = psc[...]
    meta_out[4:5, 0:4] = ppr[...]
    meta_in[POS[0, 0]] = meta_out[...]
    for load in loads:
        load.wait()
    pl.semaphore_wait(barrier, len(plane) + len(beside))

    for s in ORDER[1:]:
        k = POS[neg(s)]
        remote(meta_out, meta_in.at[k], meta_send, meta_recv.at[k], device(s[0], s[1])).start()

    def piece(slot, role, rot):
        i = slot * 3 + {"C": 0, "M": 1 + par, "O": 2 - par}[role], columns_of(role, rot)
        return hbuf.at[i], i

    half_sub = lax.broadcasted_iota(jnp.int32, (K, 128), 0)
    half_lane = lax.broadcasted_iota(jnp.int32, (K, 128), 1)

    def do_meta():
        for k in range(1, 16):
            wait_for(meta_in.at[k], meta_recv.at[k])
        wide_lane = lax.broadcasted_iota(jnp.int32, (8, 256), 1)
        rows = [jnp.zeros((8, 256), F32) for _ in range(GROUPS)]
        counts = jnp.zeros((K, 128), F32)
        score = jnp.zeros((K, 128), F32)
        prob = jnp.zeros((K, 128), F32)
        for k, s in enumerate(ORDER):
            tile = meta_in[k]
            wide = jnp.concatenate([tile, tile], axis=1)
            at = 3 * k
            g, off = at // 8, 32 * (at % 8)
            n = min(3, 8 - at % 8)
            turned = pltpu.roll(wide, off, 1) if off else wide
            rows[g] = jnp.where((wide_lane >= off) & (wide_lane < off + 32 * n), turned, rows[g])
            if n < 3:
                turned = pltpu.roll(wide, 256 - 32 * n, 1)
                rows[g + 1] = jnp.where(wide_lane < 32 * (3 - n), turned, rows[g + 1])
            sub = half_sub.astype(F32)
            for r in (1, 2):
                counts += jnp.where(tile[r : r + 1] == sub, 1.0, 0.0)
            dp = lax.rem(my + s[0], N) * N + lax.rem(mz + s[1], N)
            mine = (half_lane == half_sub - 4 * dp) & (half_lane < 4)
            score += jnp.where(mine, tile[3:4], 0.0)
            prob += jnp.where(mine, tile[4:5], 0.0)
        for g in range(GROUPS):
            trow[g] = rows[g].astype(jnp.int32)
        for i, v in enumerate((counts, score, prob)):
            cols[i] = jnp.broadcast_to(sum_lanes(v), (K, 128))

    def joined(tiles):
        top = functools.reduce(jnp.maximum, [t[0:1] for t in tiles])
        total = functools.reduce(jnp.add, [t[1:2] * jnp.exp(t[0:1] - top) for t in tiles])
        return top, total, functools.reduce(jnp.add, [t[2:3] for t in tiles])

    def run(ops):
        for op in ops:
            if op[0] == "wait":
                _, s, role, rot = op
                ref, (i, r) = piece(POS[s], role, rot)
                wait_for(ref, h_recv.at[i, r])
            elif op[0] == "send":
                _, d, role, rot, s = op
                src, _ = piece(POS[s], role, rot)
                slot = POS[s] if d[1] == "x" else POS[neg(moved(neg(s), d))]
                dst, (i, r) = piece(slot, role, rot)
                remote(src, dst, h_send, h_recv.at[i, r], toward[d]).start()
            elif op[0] == "w":
                rows = pl.ds(op[1] * 128, min(128, COLS - op[1] * 128))
                remote(
                    wt.at[rows], wbuf.at[1, rows], w_send.at[op[1]], w_recv.at[op[1]], device(dc=1)
                ).start()
            elif op[0] == "w_wait":
                if op[1] == 0:
                    own_w.wait()
                else:
                    for i in range(N_W):
                        rows = pl.ds(i * 128, min(128, COLS - i * 128))
                        wait_for(wbuf.at[1, rows], w_recv.at[i])
            elif op[0] == "meta":
                do_meta()
            elif op[0] == "merge":
                for i, v in enumerate(joined([sbuf[op[1], q] for q in range(2)])):
                    merged[op[1], i : i + 1] = v
            elif op[0] == "stat":
                k = op[1]
                at = 3 * k
                g, off = at // 8, 32 * (at % 8)
                n = min(3, 8 - at % 8)
                tile = merged[g]
                msg = (pltpu.roll(tile, 256 - off, 1) if off else tile)[:, :128]
                if n < 3:
                    msg = jnp.where(lane < 32 * n, msg, pltpu.roll(merged[g + 1], 32 * n, 1)[:, :128])
                st_out[k] = msg
                if ORDER[k] == FAR:
                    lt_in[k - EARLY, 0] = msg
            elif op[0] == "stat_send":
                k = op[1]
                s = opposite(ORDER[k])
                if k < EARLY:
                    remote(st_out.at[k], st_in.at[k], st_send, st_recv.at[k], device(s[0], s[1])).start()
                else:
                    for dx in (2, 1, 3, 0):
                        if s != (0, 0) or dx:
                            i = (k - EARLY, (N - dx) % N)
                            remote(
                                st_out.at[k], lt_in.at[i], lt_send, lt_recv.at[i], device(s[0], s[1], dx)
                            ).start()
            elif op[0] == "early":
                for k in range(EARLY):
                    wait_for(st_in.at[k], st_recv.at[k])
                for i, v in enumerate(joined([st_in[k] for k in range(EARLY)])):
                    xs_out[i : i + 1] = v
                xs_in[0] = xs_out[...]
                for dx in range(1, N):
                    remote(xs_out, xs_in.at[N - dx], xs_send, xs_recv.at[N - dx], device(dx=dx)).start()

    base = ((my * N + mz) * 8 + mx * 2) * COLS
    chunks, parts = segments()
    run(parts[0])

    steps = chunks

    def of(j, values):
        out = jnp.int32(values[0])
        for k in range(1, len(values)):
            if values[k] != values[k - 1]:
                out = jnp.where(j >= k, values[k], out)
        return out

    def step(j, _):
        pick(j, 0, len(steps), [[]] + parts[1:-1], run)
        g, w, q = (of(j, [c[i] for c in steps]) for i in range(3))
        per = 2
        wide = WIDE // 2
        rhs = jnp.concatenate(
            [hbuf[pl.ds(8 * g, 8), q * per + i].reshape(ROWS_G, 1024) for i in range(per)], axis=1
        )
        lhs = wbuf[w, :, pl.ds(pl.multiple_of(q * wide, wide), wide)]
        part = lax.dot_general(lhs, rhs, NT, preferred_element_type=F32)

        @pl.when(q == 0)
        def _():
            acc[lax.rem(g, 2), w] = part

        @pl.when(q == 1)
        def _():
            logits = acc[lax.rem(g, 2), w] + part
            row = lax.broadcasted_iota(jnp.int32, logits.shape, 0)
            target = trow[g][0:1] - (base + jnp.where(w == 0, mc, 1 - mc) * COLS)
            top = jnp.max(logits, axis=0, keepdims=True)
            sbuf[g, w, 0:1] = top
            sbuf[g, w, 1:2] = jnp.sum(jnp.exp(logits - top), axis=0, keepdims=True)
            sbuf[g, w, 2:3] = jnp.sum(jnp.where(row == target, logits, 0.0), axis=0, keepdims=True)

        return 0

    lax.fori_loop(0, len(steps), step, 0)
    run(parts[-1])

    late = [(k, dx) for k in range(16 - EARLY) for dx in range(N)]
    for k, dx in late:
        if ORDER[EARLY + k] != FAR or dx:
            wait_for(lt_in.at[k, dx], lt_recv.at[k, dx])
    for dx in range(1, N):
        wait_for(xs_in.at[dx], xs_recv.at[dx])
    top, total, picked = joined([xs_in[dx] for dx in range(N)] + [lt_in[k, dx] for k, dx in late])
    loss = top + jnp.log(total) - picked
    lo_out[...] = loss
    for dy, dz, dc in plane:
        i = POS[neg((dy, dz))] * 2 + dc
        remote(lo_out, lo_in.at[i], lo_send, lo_recv.at[i], device(dy, dz, 0, dc)).start()
    lo_in[0] = lo_out[...]
    for i in range(1, 32):
        wait_for(lo_in.at[i], lo_recv.at[i])

    sums = jnp.zeros((K, 128), F32)
    sub = half_sub.astype(F32)
    for k in range(16):
        tile = meta_in[POS[opposite(ORDER[k])]]
        for dc in range(2):
            labels = jnp.where(lax.rem(mc + dc, 2) == 0, tile[1:2], tile[2:3])
            sums += jnp.where(labels == sub, lo_in[2 * k + dc], 0.0)
    sums = jnp.broadcast_to(sum_lanes(sums), (K, 128))
    earlier, current = rates()
    score = current / earlier * cols[1] + current * (sums / cols[0]) / cols[2]
    weight = jnp.exp(score - jnp.max(score, axis=0, keepdims=True))
    probs = (1.0 - K * current) * (weight / jnp.sum(weight, axis=0, keepdims=True)) + current
    log_probs = jnp.log(probs)
    dp = my * N + mz

    def across(mask, v):
        return jnp.sum(jnp.where(mask, v, 0.0), axis=0, keepdims=True)

    out_ref[1:2] = across(half_lane == half_sub - 4 * dp, score)
    out_ref[2:3] = across(half_lane == half_sub, log_probs)
    two[2:3, 0:16] = nxt[...]
    chosen = across(two[2:3, :128] == half_sub, probs)
    out_ref[3:4] = 1.0 / (K * chosen)
    own = 2 * POS[2, 2]
    loss = jnp.where(mx // 2 == mc, lo_in[own], lo_in[own + 1])
    loss = jnp.broadcast_to(loss, (8, 128))
    out = loss
    for q in range(1, 4):
        out = jnp.where(2 * lax.rem(mx, 2) + mc == q, pltpu.roll(loss, 128 - 24 * q, 1), out)
    out_ref[0:1] = out[0:1]

    wait_for(hbuf.at[pl.ds(0, 45)], h_send)
    for i in range(N_W):
        rows = pl.ds(i * 128, min(128, COLS - i * 128))
        wait_for(wbuf.at[1, rows], w_send.at[i])
    wait_for(meta_in.at[pl.ds(0, 15)], meta_send)
    wait_for(st_in.at[pl.ds(0, EARLY)], st_send)
    wait_for(st_in.at[pl.ds(0, 11)], lt_send)
    wait_for(xs_in.at[pl.ds(0, 3)], xs_send)
    wait_for(lo_in.at[pl.ds(0, 31)], lo_send)


def finish(rows, *outs):
    for i, out in enumerate(outs):
        out[...] = rows[i : i + 1, : out.shape[1]]


def body(hidden, output_weight, targets, labels, prev_scores, prev_probs, next_domains):
    dma = pltpu.SemaphoreType.DMA
    vmem = pl.BlockSpec(memory_space=pltpu.VMEM)
    rows = pl.pallas_call(
        kernel,
        out_shape=jax.ShapeDtypeStruct((8, 128), F32),
        in_specs=[pl.BlockSpec(memory_space=pl.ANY)] * 2 + [vmem] * 5,
        out_specs=vmem,
        scratch_shapes=[
            pltpu.VMEM((48, 4, 32, 1024), jnp.bfloat16),
            pltpu.VMEM((2, COLS, WIDE), jnp.bfloat16),
            pltpu.VMEM((2, 2, COLS, ROWS_G), F32),
            pltpu.VMEM((8, 128), F32),
            pltpu.VMEM((16, 8, 128), F32),
            pltpu.VMEM((8, 256), jnp.int32),
            pltpu.VMEM((GROUPS, 8, 256), jnp.int32),
            pltpu.VMEM((3, K, 128), F32),
            pltpu.VMEM((GROUPS, 2, 8, 256), F32),
            pltpu.VMEM((GROUPS, 8, 256), F32),
            pltpu.VMEM((16, 8, 128), F32),
            pltpu.VMEM((16, 8, 128), F32),
            pltpu.VMEM((16 - EARLY, N, 8, 128), F32),
            pltpu.VMEM((8, 128), F32),
            pltpu.VMEM((N, 8, 128), F32),
            pltpu.VMEM((1, 128), F32),
            pltpu.VMEM((32, 1, 128), F32),
            dma((12,)),
            dma(()),
            dma(()),
            dma((48, 4)),
            dma((N_W,)),
            dma((N_W,)),
            dma(()),
            dma((16,)),
            dma(()),
            dma((16,)),
            dma(()),
            dma((16 - EARLY, N)),
            dma(()),
            dma((N,)),
            dma(()),
            dma((32,)),
        ],
        compiler_params=pltpu.CompilerParams(
            collective_id=0, has_side_effects=True, vmem_limit_bytes=56 * 1024 * 1024
        ),
    )(
        hidden,
        output_weight.T,
        targets.reshape(1, -1),
        labels.reshape(1, -1),
        prev_scores.reshape(1, -1),
        prev_probs.reshape(1, -1),
        next_domains.reshape(1, -1),
    )
    sizes = (24, 4, K, 16)
    outs = pl.pallas_call(
        finish,
        out_shape=[jax.ShapeDtypeStruct((1, n), F32) for n in sizes],
        in_specs=[vmem],
        out_specs=[vmem] * 4,
    )(rows)
    return tuple(o.reshape(-1) for o in outs)


def solution(mesh):
    torus = Mesh(mesh.devices.reshape(N, N, N, 2), ALL)
    return jax.shard_map(
        body,
        mesh=torus,
        in_specs=(P(DP, None), P(None, ALL), P(DP), P(DP, None), P(DP), P(DP), P(DP)),
        out_specs=(P(ALL), P(DP), P(), P(DP)),
        check_vma=False,
    )
```
